256 devices in a mesh: mem: 32 (over z_hi, y, core), lat: 8 (over z_lo, x).
Axes of the slice: x: 4, y: 4, z: 8 (z_hi: 4, z_lo: 2; z = z_hi * 2 + z_lo), core: 2. Of those that a mesh axis runs over, the one named last changes fastest.
Arguments:
- controls: bfloat16 [128, 64, 256, 256], P('mem', None, 'lat'), may hold values from -6 to 6
- spread: bfloat16 [128, 64, 256, 256], P('mem', None, 'lat'), may hold values from -1.5 to 1.5
- classes: int32 [256, 256], P('lat'), may hold values from 0 to 7
- prec_table: float32 [8, 64], replicated, may hold values from 0.25 to 4
- vert_loc: bfloat16 [64, 64], replicated, may hold values from 0 to 1
- lon_loc: bfloat16 [256, 256], replicated, may hold values from 0 to 1
- lat_loc: bfloat16 [256, 256], replicated, may hold values from 0 to 1
Outputs:
- localized: bfloat16 [128, 64, 256, 256], P('mem', None, 'lat')
The draws below stay inside these ranges and needn't reach their ends.
All inputs are finite; a program needn't handle non-finite values.
Results may differ from the reference program's by a relative error of at most 0.0064.
Values may be sent and summed in bfloat16 or wider, within the bound.
No kernel may reach another device: no remote copies, remote signals or barrier semaphores. Data moves between devices by JAX's collectives and lax.ppermute only.
A program may use at most 128 MiB of HBM per device.

```python
import math
import jax
import jax.numpy as jnp
from jax import lax

LEV = 64
LAT = 256
LON = 256
NCLASS = 8
MEMBERS = 128


def draw_range():
    return (0.5, 1.5, 0.6)


def banded(key, size, reach):
    lower, upper, centre = draw_range()
    positions = jnp.arange(size)
    distance = jnp.abs(positions[:, None] - positions[None, :]).astype(jnp.float32)
    noise = jax.random.uniform(key, (size, size), jnp.float32, lower, upper)
    offdiag = jnp.exp(-distance / float(reach)) * noise / (4.0 * float(reach))
    return jnp.where(distance == 0.0, centre + 0.05 * noise, offdiag)


def draw_vert_loc(key, part):
    return banded(jax.random.fold_in(key, 11), LEV, LEV // 4).astype(jnp.bfloat16)


def draw_lon_loc(key, part):
    return banded(jax.random.fold_in(key, 23), LON, LON // 4).astype(jnp.bfloat16)


def draw_lat_loc(key, part):
    return banded(jax.random.fold_in(key, 37), LAT, LAT // 4).astype(jnp.bfloat16)


def plant(array, own_key, smallest, top_value):
    longest = array.shape.index(max(array.shape))
    spots = []
    for shift in (0, 1):
        where = [jax.random.randint(jax.random.fold_in(own_key, axis), (), 0, length) for axis, length in enumerate(array.shape)]
        where[longest] = (where[longest] + shift) % array.shape[longest]
        spots.append(tuple(where))
    return array.at[spots[0]].set(smallest).at[spots[1]].set(top_value)


def steps_of(key, dims, pieces, low, largest):
    def one(axis_at, parts):
        heights = jax.random.uniform(jax.random.fold_in(jax.random.fold_in(key, 6), axis_at), (parts,), jnp.float32, low / len(pieces), largest / len(pieces))
        return jnp.repeat(jnp.exp(heights), dims[axis_at] // parts).reshape((-1,) + (1,) * (len(dims) - axis_at - 1))

    factor_of = one(*pieces[0])
    for cut in pieces[1:]:
        factor_of = factor_of * one(*cut)
    return factor_of


def normal_values(key, shape, width, most, shards=(), kind=jnp.bfloat16):
    values = width * jax.random.normal(key, shape, jnp.float32)
    if shards:
        values = values * steps_of(key, shape, shards, -0.22, 0.18)
    return jnp.clip(values, -most, most).astype(kind)


def setup_inputs(seed: int = 0) -> dict:
    key_of = jax.random.split(jax.random.key(seed), 8)
    controls = normal_values(key_of[0], (MEMBERS, LEV, LAT, LON), 1.0, 6.0, ((0, 32), (2, 8)))
    spread = normal_values(key_of[1], (MEMBERS, LEV, LAT, LON), 0.25, 1.5, ((0, 32), (2, 8)))
    classes = plant(jax.random.randint(key_of[2], (LAT, LON), 0, NCLASS), jax.random.fold_in(key_of[2], 1), 0, NCLASS - 1).astype(jnp.int32)
    prec_table = jnp.clip(jnp.exp(jax.random.uniform(key_of[3], (NCLASS, LEV), jnp.float32, math.log(0.25), math.log(4.0))), 0.25, 4.0)
    vert_loc = draw_vert_loc(jax.random.fold_in(key_of[7], 71), 0)
    lon_loc = draw_lon_loc(jax.random.fold_in(key_of[7], 71), 0)
    lat_loc = draw_lat_loc(jax.random.fold_in(key_of[7], 71), 0)
    return dict(controls=controls, spread=spread, classes=classes, prec_table=prec_table, vert_loc=vert_loc, lon_loc=lon_loc, lat_loc=lat_loc)


def lookup(table, classes):
    numbers = jnp.arange(table.shape[0], dtype=jnp.int32)
    onehot = (classes[None, :, :] == numbers[:, None, None]).astype(jnp.float32)
    return jnp.einsum("kl,kab->lab", table, onehot, precision=lax.Precision.HIGHEST)


def reference(controls, spread, classes, prec_table, vert_loc, lon_loc, lat_loc):
    def accumulate(total, pair):
        member_spread, member_ctrl = pair
        return total + member_spread.astype(jnp.float32) * member_ctrl.astype(jnp.float32), None

    start = jnp.zeros(controls.shape[1:], jnp.float32)
    increment, _ = lax.scan(accumulate, start, (spread, controls))
    weighted = increment * lookup(prec_table, classes)
    vert_f = vert_loc.astype(jnp.float32)
    lon_f = lon_loc.astype(jnp.float32)
    lat_f = lat_loc.astype(jnp.float32)

    def member(member_spread):
        adjoint = (member_spread.astype(jnp.float32) * weighted).astype(jnp.bfloat16)
        along_lon = jnp.einsum("lac,bc->lab", adjoint.astype(jnp.float32), lon_f, precision=lax.Precision.HIGHEST).astype(jnp.bfloat16)
        along_lev = jnp.einsum("lj,jab->lab", vert_f, along_lon.astype(jnp.float32), precision=lax.Precision.HIGHEST).astype(jnp.bfloat16)
        return jnp.einsum("ac,lcb->lba", lat_f, along_lev.astype(jnp.float32), precision=lax.Precision.HIGHEST).astype(jnp.bfloat16)

    return lax.map(member, spread)
```

```python
import functools

import jax
import jax.numpy as jnp
from jax import lax
from jax.experimental import pallas as pl
from jax.experimental.pallas import tpu as pltpu
from jax.sharding import Mesh
from jax.sharding import PartitionSpec as P

F32 = jnp.float32
BF16 = jnp.bfloat16
ZH, Y, CORE = 4, 4, 2
LATS = 8
RING = ("zh", "y")
LAT = "lat"
EACH = 4


def nt_dot(a, b):
    return lax.dot_general(a, b, (((1,), (1,)), ((), ())), preferred_element_type=F32)


def compiler_params(mib):
    return pltpu.CompilerParams(
        dimension_semantics=("arbitrary",), vmem_limit_bytes=mib * 1024 * 1024
    )


def half_sum_kernel(start_ref, spread_ref, controls_ref, *rest):
    out_ref = rest[-1]
    total = spread_ref[0].astype(F32) * controls_ref[0].astype(F32)
    for k in range(1, spread_ref.shape[0]):
        total += spread_ref[k].astype(F32) * controls_ref[k].astype(F32)
    if len(rest) == 2:
        total += rest[0][...].astype(F32)
    out_ref[...] = total.astype(BF16)


def half_sum(spread, controls, half, arrived=None):
    members, levels, rows, cols = spread.shape
    step = 8
    count = levels // 2 // step
    field = pl.BlockSpec((members, step, rows, cols), lambda i, s: (0, s[0] * count + i, 0, 0))
    piece = pl.BlockSpec((step, rows, cols), lambda i, s: (i, 0, 0))
    args = (spread, controls) if arrived is None else (spread, controls, arrived)
    return pl.pallas_call(
        half_sum_kernel,
        grid_spec=pltpu.PrefetchScalarGridSpec(
            num_scalar_prefetch=1,
            grid=(count,),
            in_specs=[field, field] + [piece] * (len(args) - 2),
            out_specs=piece,
        ),
        out_shape=jax.ShapeDtypeStruct((levels // 2, rows, cols), BF16),
        compiler_params=compiler_params(8),
        name="half_sum",
    )(half, *args)


def tables_kernel(me_ref, vert_ref, lat_ref, big_ref, turned_ref):
    levels = vert_ref.shape[0]
    size = levels * 8
    row = lax.broadcasted_iota(jnp.int32, (size, levels), 0) >> 3
    col = lax.broadcasted_iota(jnp.int32, (size, levels), 1)
    source = (row & ~3) | ((row + 8 - me_ref[0]) & 3)
    pick_out = jnp.where(source == col, 1.0, 0.0).astype(BF16)
    pick_in = jnp.where(row == col, 1.0, 0.0).astype(BF16)
    tall = jnp.dot(pick_out, vert_ref[...], preferred_element_type=F32).astype(BF16)
    wide = nt_dot(tall, pick_in)
    r = lax.broadcasted_iota(jnp.int32, (size, size), 0) & 7
    c = lax.broadcasted_iota(jnp.int32, (size, size), 1) & 7
    big_ref[...] = jnp.where(r == c, wide, 0.0).astype(BF16)
    for part in range(2):
        block = lat_ref[:, 128 * part : 128 * part + 128].astype(F32)
        for turn in range(EACH):
            moved = block if turn == 0 else pltpu.roll(block, 32 * turn, 1)
            turned_ref[turn, :, 128 * part : 128 * part + 128] = moved.astype(BF16)


def tables(me, vert_loc, lat_loc):
    levels = vert_loc.shape[0]
    size = lat_loc.shape[0]
    return pl.pallas_call(
        tables_kernel,
        in_specs=[
            pl.BlockSpec(memory_space=pltpu.SMEM),
            pl.BlockSpec(memory_space=pltpu.VMEM),
            pl.BlockSpec(memory_space=pltpu.VMEM),
        ],
        out_specs=[pl.BlockSpec(memory_space=pltpu.VMEM)] * 2,
        out_shape=[
            jax.ShapeDtypeStruct((levels * 8, levels * 8), BF16),
            jax.ShapeDtypeStruct((EACH, size, size), BF16),
        ],
        compiler_params=pltpu.CompilerParams(vmem_limit_bytes=16 * 1024 * 1024),
        name="tables",
    )(me, vert_loc, lat_loc)


def spread_out_kernel(half_ref, spread_ref, own_ref, other_ref, big_ref, lon_ref, out_ref, adj, mixed):
    levels, rows, cols = adj.shape
    half = levels // 2
    for which, piece in ((0, own_ref), (1, other_ref)):
        base = (half_ref[0] ^ which) * half

        @pl.loop(0, half)
        def _(i):
            adj[base + i] = spread_ref[0, base + i].astype(F32) * piece[i].astype(F32)

    for g in range(rows // 8):
        x = adj[:, 8 * g : 8 * g + 8, :].reshape(levels * 8, cols).astype(BF16)
        y = jnp.dot(big_ref[...], x, preferred_element_type=F32)
        mixed[:, 8 * g : 8 * g + 8, :] = y.reshape(levels, 8, cols)
    for n in range(levels * rows // 256):
        at = 256 // rows
        x = mixed[at * n : at * n + at].reshape(256, cols).astype(BF16)
        y = nt_dot(lon_ref[...], x).astype(BF16)
        out_ref[:, 0, :, 256 * n : 256 * n + 256] = y.reshape(LATS, cols // LATS, 256)


def spread_out(half, spread, own, other, big, lon_loc):
    members, levels, rows, cols = spread.shape
    share = cols // LATS

    def whole(x):
        return pl.BlockSpec(x.shape, lambda k, s: (0,) * x.ndim)

    return pl.pallas_call(
        spread_out_kernel,
        grid_spec=pltpu.PrefetchScalarGridSpec(
            num_scalar_prefetch=1,
            grid=(members,),
            in_specs=[
                pl.BlockSpec((1, levels, rows, cols), lambda k, s: (k, 0, 0, 0)),
                whole(own),
                whole(other),
                whole(big),
                whole(lon_loc),
            ],
            out_specs=pl.BlockSpec((LATS, 1, share, levels * rows), lambda k, s: (0, k, 0, 0)),
            scratch_shapes=[pltpu.VMEM((levels, rows, cols), F32)] * 2,
        ),
        out_shape=jax.ShapeDtypeStruct((LATS, members, share, levels * rows), BF16),
        compiler_params=compiler_params(24),
        name="spread_out",
    )(half, spread, own, other, big, lon_loc)


def finish_kernel(parts_ref, turned_ref, out_ref):
    share = parts_ref.shape[2]
    groups = parts_ref.shape[3] // 128
    lane = lax.broadcasted_iota(jnp.int32, (share, 128), 1) >> 5
    at = [lane == q for q in range(3)]
    for turn in range(EACH):
        lines = []
        for g in range(groups):
            sides = []
            for part in range(2):
                tiles = [
                    parts_ref[EACH * part + (q - turn) % EACH, 0, :, 128 * g : 128 * g + 128]
                    for q in range(EACH)
                ]
                side = tiles[3]
                for q in range(3):
                    side = jnp.where(at[q], tiles[q], side)
                sides.append(side)
            lines.append(jnp.concatenate(sides, axis=1))
        x = jnp.concatenate(lines, axis=0)
        y = nt_dot(x, turned_ref[turn]).astype(BF16)
        for g in range(groups):
            out_ref[0, EACH * g + turn] = y[share * g : share * g + share]


def finish(parts, turned):
    _, members, share, wide = parts.shape
    size = turned.shape[1]
    levels = wide // 32
    return pl.pallas_call(
        finish_kernel,
        grid=(members,),
        in_specs=[
            pl.BlockSpec((LATS, 1, share, wide), lambda k: (0, k, 0, 0)),
            pl.BlockSpec(turned.shape, lambda k: (0, 0, 0)),
        ],
        out_specs=pl.BlockSpec((1, levels, share, size), lambda k: (k, 0, 0, 0)),
        out_shape=jax.ShapeDtypeStruct((members, levels, share, size), BF16),
        compiler_params=compiler_params(16),
        name="finish",
    )(parts, turned)


def weigh_kernel(first_ref, pieces_ref, classes_ref, table_ref, out_ref):
    peers, each = pieces_ref.shape[:2]
    classes = classes_ref[...]
    for l in range(each):
        total = pieces_ref[0, l].astype(F32)
        for n in range(1, peers):
            total += pieces_ref[n, l].astype(F32)
        precision = jnp.full(classes.shape, table_ref[0, first_ref[0] + l], F32)
        for n in range(1, table_ref.shape[0]):
            precision = jnp.where(classes == n, table_ref[n, first_ref[0] + l], precision)
        weighted = (total * precision).astype(BF16)
        for n in range(peers):
            out_ref[n, l] = weighted


def weigh(first, pieces, classes, prec_table):
    vmem = pl.BlockSpec(memory_space=pltpu.VMEM)
    smem = pl.BlockSpec(memory_space=pltpu.SMEM)
    return pl.pallas_call(
        weigh_kernel,
        in_specs=[smem, vmem, vmem, smem],
        out_specs=vmem,
        out_shape=jax.ShapeDtypeStruct(pieces.shape, BF16),
        compiler_params=pltpu.CompilerParams(vmem_limit_bytes=8 * 1024 * 1024),
        name="weigh",
    )(first, pieces, classes, prec_table)


def local(controls, spread, classes, prec_table, vert_loc, lon_loc, lat_loc):
    levels = spread.shape[1]
    controls = pltpu.with_memory_space_constraint(controls, pltpu.HBM)
    spread = pltpu.with_memory_space_constraint(spread, pltpu.HBM)
    core = lax.axis_index("core")
    own_half = core.reshape(1)
    other_half = (1 - core).reshape(1)
    me = lax.axis_index(LAT).reshape(1)
    swap = [(0, 1), (1, 0)]

    big, turned = tables(me, vert_loc, lat_loc)
    arrived = lax.ppermute(half_sum(spread, controls, other_half), "core", swap)
    chip = half_sum(spread, controls, own_half, arrived)
    peers = ZH * Y
    each = levels // (CORE * peers)
    pieces = lax.all_to_all(
        chip.reshape(peers, each, *chip.shape[1:]), RING, split_axis=0, concat_axis=0, tiled=True
    )
    first = ((core * peers + lax.axis_index(RING)) * each).reshape(1)
    copies = weigh(first, pieces, classes, prec_table)
    own = lax.all_to_all(copies, RING, split_axis=0, concat_axis=0, tiled=True).reshape(chip.shape)
    other = lax.ppermute(own, "core", swap)
    sending = spread_out(own_half, spread, own, other, big, lon_loc)
    parts = lax.all_to_all(sending, LAT, split_axis=0, concat_axis=0, tiled=True)
    return finish(parts, turned)


def solution(mesh):
    finer = Mesh(
        mesh.devices.reshape(ZH, Y, CORE, mesh.shape["lat"]), ("zh", "y", "core", LAT)
    )
    members = P(("zh", "y", "core"), None, LAT, None)
    return jax.shard_map(
        local,
        mesh=finer,
        in_specs=(members, members, P(LAT, None), P(), P(), P(), P()),
        out_specs=members,
        check_vma=False,
    )
```

```python
import jax
import jax.numpy as jnp
from jax import lax
from jax.experimental import pallas as pl
from jax.experimental.pallas import tpu as pltpu
from jax.sharding import Mesh
from jax.sharding import PartitionSpec as P

F32 = jnp.float32
BF16 = jnp.bfloat16
ZH, Y, CORE = 4, 4, 2
LATS = 8
LAT = "lat"
EACH = 4
GROUPS = ((0, 2), (2, 2))


def nt_dot(a, b):
    return lax.dot_general(a, b, (((1,), (1,)), ((), ())), preferred_element_type=F32)


def compiler_params(mib):
    return pltpu.CompilerParams(
        dimension_semantics=("arbitrary",), vmem_limit_bytes=mib * 1024 * 1024
    )


def half_sum_kernel(start_ref, spread_ref, controls_ref, *rest):
    outs = rest
    if len(rest) > 1:
        outs = rest[1:]
    at = pl.program_id(0)
    pieces = []
    for l in range(spread_ref.shape[1]):
        total = spread_ref[0, l].astype(F32) * controls_ref[0, l].astype(F32)
        for k in range(1, spread_ref.shape[0]):
            total += spread_ref[k, l].astype(F32) * controls_ref[k, l].astype(F32)
        if len(rest) > 1:
            total += rest[0][0, l].astype(F32)
            for d, out in enumerate(outs):

                @pl.when(at == d)
                def _(out=out, total=total, l=l):
                    out[l] = total.astype(out.dtype)
        else:
            outs[0][0, l] = total.astype(BF16)


def half_sum(spread, controls, start, arrived=None):
    members, levels, rows, cols = spread.shape
    step = levels // (CORE * Y)
    field = pl.BlockSpec(
        (members, step, rows, cols), lambda d, s: (0, s[0] * Y + ((s[1] + d) & (Y - 1)), 0, 0)
    )
    piece = pl.BlockSpec((1, step, rows, cols), lambda d, s: (d, 0, 0, 0))
    whole = pl.BlockSpec((step, rows, cols), lambda d, s: (0, 0, 0))
    if arrived is None:
        args, in_specs, out_specs = (spread, controls), [field, field], piece
        out_shape = jax.ShapeDtypeStruct((Y, step, rows, cols), BF16)
    else:
        args, in_specs, out_specs = (spread, controls, arrived), [field, field, piece], [whole] * Y
        out_shape = [
            jax.ShapeDtypeStruct((step, rows, cols), BF16 if d else F32) for d in range(Y)
        ]
    return pl.pallas_call(
        half_sum_kernel,
        grid_spec=pltpu.PrefetchScalarGridSpec(
            num_scalar_prefetch=1, grid=(Y,), in_specs=in_specs, out_specs=out_specs
        ),
        out_shape=out_shape,
        compiler_params=compiler_params(8),
        name="half_sum",
    )(start, *args)


def tables_kernel(me_ref, vert_ref, lon_ref, lat_ref, big_ref, lon_out_ref, turned_ref):
    me = me_ref[0]
    levels = vert_ref.shape[0]
    size = levels * 8
    row = lax.broadcasted_iota(jnp.int32, (size, levels), 0) >> 3
    col = lax.broadcasted_iota(jnp.int32, (size, levels), 1)
    source = (row & ~3) | ((row + 8 - me) & 3)
    pick_out = jnp.where(source == col, 1.0, 0.0).astype(BF16)
    pick_in = jnp.where(row == col, 1.0, 0.0).astype(BF16)
    tall = jnp.dot(pick_out, vert_ref[...], preferred_element_type=F32).astype(BF16)
    wide = nt_dot(tall, pick_in)
    r = lax.broadcasted_iota(jnp.int32, (size, size), 0) & 7
    c = lax.broadcasted_iota(jnp.int32, (size, size), 1) & 7
    big_ref[...] = jnp.where(r == c, wide, 0.0).astype(BF16)
    share = lon_ref.shape[0] // LATS
    for d in range(LATS):
        at = pl.multiple_of(((me + d) & (LATS - 1)) * share, share)
        lon_out_ref[share * d : share * d + share, :] = lon_ref[pl.ds(at, share), :]
    rows = lat_ref.shape[0]
    from_col = lax.broadcasted_iota(jnp.int32, (rows, rows), 0)
    to_col = lax.broadcasted_iota(jnp.int32, (rows, rows), 1)
    for turn in range(EACH):
        back = EACH * (to_col >> 7) + ((turn - (to_col >> 5)) & 3)
        want = (((me + 16 - back) & (LATS - 1)) << 5) | (to_col & 31)
        move = jnp.where(from_col == want, 1.0, 0.0).astype(BF16)
        turned_ref[turn] = jnp.dot(
            lat_ref[...], move, preferred_element_type=F32
        ).astype(BF16)


def tables(me, vert_loc, lon_loc, lat_loc):
    levels = vert_loc.shape[0]
    size = lat_loc.shape[0]
    return pl.pallas_call(
        tables_kernel,
        in_specs=[pl.BlockSpec(memory_space=pltpu.SMEM)]
        + [pl.BlockSpec(memory_space=pltpu.VMEM)] * 3,
        out_specs=[pl.BlockSpec(memory_space=pltpu.VMEM)] * 3,
        out_shape=[
            jax.ShapeDtypeStruct((levels * 8, levels * 8), BF16),
            jax.ShapeDtypeStruct(lon_loc.shape, BF16),
            jax.ShapeDtypeStruct((EACH, size, size), BF16),
        ],
        compiler_params=pltpu.CompilerParams(vmem_limit_bytes=16 * 1024 * 1024),
        cost_estimate=pl.CostEstimate(
            flops=600_000_000, bytes_accessed=2_000_000, transcendentals=0
        ),
        name="tables",
    )(me, vert_loc, lon_loc, lat_loc)


def join_kernel(*refs):
    *pieces, out_ref = refs
    for l in range(out_ref.shape[0]):
        total = pieces[0][l].astype(F32)
        for piece in pieces[1:]:
            total += piece[l].astype(F32)
        out_ref[l] = total.astype(BF16)


def join(pieces):
    vmem = pl.BlockSpec(memory_space=pltpu.VMEM)
    return pl.pallas_call(
        join_kernel,
        in_specs=[vmem] * len(pieces),
        out_specs=vmem,
        out_shape=jax.ShapeDtypeStruct(pieces[0].shape, BF16),
        compiler_params=pltpu.CompilerParams(vmem_limit_bytes=8 * 1024 * 1024),
        name="join",
    )(*pieces)


def weigh_kernel(first_ref, classes_ref, table_ref, *refs):
    *pieces, out_ref = refs
    classes = classes_ref[...]
    numbers = range(1, table_ref.shape[0])
    at = [classes == n for n in numbers]
    for l in range(out_ref.shape[0]):
        total = pieces[0][l].astype(F32)
        for piece in pieces[1:]:
            total += piece[l].astype(F32)
        precision = jnp.full(classes.shape, table_ref[0, first_ref[0] + l], F32)
        for n in numbers:
            precision = jnp.where(at[n - 1], table_ref[n, first_ref[0] + l], precision)
        out_ref[l] = (total * precision).astype(BF16)


def weigh(first, classes, prec_table, pieces):
    vmem = pl.BlockSpec(memory_space=pltpu.VMEM)
    smem = pl.BlockSpec(memory_space=pltpu.SMEM)
    return pl.pallas_call(
        weigh_kernel,
        in_specs=[smem, vmem, smem] + [vmem] * len(pieces),
        out_specs=vmem,
        out_shape=jax.ShapeDtypeStruct(pieces[0].shape, BF16),
        compiler_params=pltpu.CompilerParams(vmem_limit_bytes=8 * 1024 * 1024),
        name="weigh",
    )(first, classes, prec_table, *pieces)


def spread_out_kernel(start_ref, spread_ref, *refs):
    weights = refs[: CORE * Y]
    big_ref, lon_ref = refs[CORE * Y : CORE * Y + 2]
    outs = refs[CORE * Y + 2 : CORE * Y + 2 + LATS]
    adj, mixed = refs[CORE * Y + 2 + LATS :]
    levels, rows, cols = adj.shape
    step = levels // (CORE * Y)
    for n, piece in enumerate(weights):
        core = start_ref[0] ^ (n // Y)
        base = (core * Y + ((start_ref[1] - n % Y) & (Y - 1))) * step
        for i in range(step):
            adj[base + i] = spread_ref[0, base + i].astype(F32) * piece[i].astype(F32)
    for g in range(rows // 8):
        x = adj[:, 8 * g : 8 * g + 8, :].reshape(levels * 8, cols).astype(BF16)
        y = jnp.dot(big_ref[...], x, preferred_element_type=F32)
        mixed[:, 8 * g : 8 * g + 8, :] = y.reshape(levels, 8, cols)
    share = cols // LATS
    for n in range(levels * rows // 256):
        at = 256 // rows
        x = mixed[at * n : at * n + at].reshape(256, cols).astype(BF16)
        y = nt_dot(lon_ref[...], x).astype(BF16)
        for d, out in enumerate(outs):
            out[0, :, 256 * n : 256 * n + 256] = y[share * d : share * d + share]


def spread_out(start, spread, weights, big, lon, first, count):
    _, levels, rows, cols = spread.shape
    share = cols // LATS

    def whole(x):
        return pl.BlockSpec(x.shape, lambda k, s: (0,) * x.ndim)

    return pl.pallas_call(
        spread_out_kernel,
        grid_spec=pltpu.PrefetchScalarGridSpec(
            num_scalar_prefetch=1,
            grid=(count,),
            in_specs=[pl.BlockSpec((1, levels, rows, cols), lambda k, s: (first + k, 0, 0, 0))]
            + [whole(x) for x in (*weights, big, lon)],
            out_specs=[pl.BlockSpec((1, share, levels * rows), lambda k, s: (k, 0, 0))] * LATS,
            scratch_shapes=[pltpu.VMEM((levels, rows, cols), F32)] * 2,
        ),
        out_shape=[jax.ShapeDtypeStruct((count, share, levels * rows), BF16)] * LATS,
        compiler_params=compiler_params(24),
        cost_estimate=pl.CostEstimate(
            flops=count * 1_500_000_000, bytes_accessed=count * 2_500_000, transcendentals=0
        ),
        name="spread_out",
    )(start, spread, *weights, big, lon)


def finish_kernel(me_ref, *refs):
    parts = refs[:LATS]
    turned_ref, out_ref = refs[LATS], refs[-1]
    share = parts[0].shape[1]
    groups = parts[0].shape[2] // 128
    lane = lax.broadcasted_iota(jnp.int32, (share, 128), 1) >> 5
    at = [lane == q for q in range(3)]
    for turn in range(EACH):
        lines = []
        for g in range(groups):
            sides = []
            for part in range(2):
                tiles = [
                    parts[EACH * part + (turn - q) % EACH][0, :, 128 * g : 128 * g + 128]
                    for q in range(EACH)
                ]
                side = tiles[3]
                for q in range(3):
                    side = jnp.where(at[q], tiles[q], side)
                sides.append(side)
            lines.append(jnp.concatenate(sides, axis=1))
        x = jnp.concatenate(lines, axis=0)
        y = nt_dot(x, turned_ref[turn]).astype(BF16)
        level = (turn + 8 - me_ref[0]) & 3
        for g in range(groups):
            out_ref[0, EACH * g + level] = y[share * g : share * g + share]


def finish(me, parts, turned, first, members, so_far=None):
    count, share, wide = parts[0].shape
    size = turned.shape[1]
    levels = wide // 32
    args = (*parts, turned) if so_far is None else (*parts, turned, so_far)
    extra = [] if so_far is None else [pl.BlockSpec(memory_space=pl.ANY)]
    return pl.pallas_call(
        finish_kernel,
        grid_spec=pltpu.PrefetchScalarGridSpec(
            num_scalar_prefetch=1,
            grid=(count,),
            in_specs=[pl.BlockSpec((1, share, wide), lambda k, s: (k, 0, 0))] * LATS
            + [pl.BlockSpec(turned.shape, lambda k, s: (0, 0, 0))]
            + extra,
            out_specs=pl.BlockSpec((1, levels, share, size), lambda k, s: (first + k, 0, 0, 0)),
        ),
        out_shape=jax.ShapeDtypeStruct((members, levels, share, size), BF16),
        input_output_aliases={} if so_far is None else {len(args): 0},
        compiler_params=compiler_params(16),
        cost_estimate=pl.CostEstimate(
            flops=count * 700_000_000, bytes_accessed=count * 2_500_000, transcendentals=0
        ),
        name="finish",
    )(me, *args)


def onward(n, d):
    return [(i, (i + d) % n) for i in range(n)]


def local(controls, spread, classes, prec_table, vert_loc, lon_loc, lat_loc):
    controls = pltpu.with_memory_space_constraint(controls, pltpu.HBM)
    spread = pltpu.with_memory_space_constraint(spread, pltpu.HBM)
    members, levels = spread.shape[:2]
    core, y = lax.axis_index("core"), lax.axis_index("y")
    here = jnp.stack([core, y])
    me = lax.axis_index(LAT).reshape(1)
    first = ((core * Y + y) * (levels // (CORE * Y))).reshape(1)
    swap = [(0, 1), (1, 0)]

    big, lon, turned = tables(me, vert_loc, lon_loc, lat_loc)
    arrived = lax.ppermute(half_sum(spread, controls, jnp.stack([1 - core, y])), "core", swap)
    pieces = half_sum(spread, controls, here, arrived)
    along_y = join([pieces[0]] + [lax.ppermute(pieces[d], "y", onward(Y, d)) for d in range(1, Y)])
    along_z = [along_y] + [lax.ppermute(along_y, "zh", onward(ZH, d)) for d in range(1, ZH)]
    weighted = weigh(first, classes, prec_table, along_z)
    own = [weighted] + [lax.ppermute(weighted, "y", onward(Y, d)) for d in range(1, Y)]
    weights = own + [lax.ppermute(x, "core", swap) for x in own]

    result = None
    for start, count in GROUPS:
        sending = spread_out(here, spread, weights, big, lon, start, count)
        parts = [sending[0]] + [
            lax.ppermute(sending[d], LAT, onward(LATS, d)) for d in range(1, LATS)
        ]
        result = finish(me, parts, turned, start, members, result)
    return result


def solution(mesh):
    finer = Mesh(
        mesh.devices.reshape(ZH, Y, CORE, mesh.shape["lat"]), ("zh", "y", "core", LAT)
    )
    members = P(("zh", "y", "core"), None, LAT, None)
    return jax.shard_map(
        local,
        mesh=finer,
        in_specs=(members, members, P(LAT, None), P(), P(), P(), P()),
        out_specs=members,
        check_vma=False,
    )
```

```python
import jax
import jax.numpy as jnp
from jax import lax
from jax.experimental import pallas as pl
from jax.experimental.pallas import tpu as pltpu
from jax.sharding import Mesh
from jax.sharding import PartitionSpec as P


F32 = jnp.float32
BF16 = jnp.bfloat16
ZH, Y, CORE = 4, 4, 2
LATS = 8
LAT = "lat"
EACH = 4
GROUPS = ((0, 2), (2, 2))
ORDER = (6, 2, 4, 5, 7, 1, 3)


def nt_dot(a, b):
    return lax.dot_general(a, b, (((1,), (1,)), ((), ())), preferred_element_type=F32)


def compiler_params(mib):
    return pltpu.CompilerParams(
        dimension_semantics=("arbitrary",), vmem_limit_bytes=mib * 1024 * 1024
    )


def own_sum_kernel(start_ref, spread_ref, controls_ref, send_ref, keep_ref):
    at = pl.program_id(0)
    for l in range(spread_ref.shape[1]):
        total = spread_ref[0, l].astype(F32) * controls_ref[0, l].astype(F32)
        for k in range(1, spread_ref.shape[0]):
            total += spread_ref[k, l].astype(F32) * controls_ref[k, l].astype(F32)

        @pl.when(at < Y)
        def _(total=total, l=l):
            send_ref[0, l] = total.astype(BF16)

        @pl.when(at >= Y)
        def _(total=total, l=l):
            keep_ref[0, l] = total


def own_sum(spread, controls, start):
    members, levels, rows, cols = spread.shape
    step = levels // (CORE * Y)

    def source(i, s):
        half = s[0] ^ jnp.where(i < Y, 1, 0)
        return (0, half * Y + ((s[1] + i) & (Y - 1)), 0, 0)

    field = pl.BlockSpec((members, step, rows, cols), source)
    block = (1, step, rows, cols)
    return pl.pallas_call(
        own_sum_kernel,
        grid_spec=pltpu.PrefetchScalarGridSpec(
            num_scalar_prefetch=1,
            grid=(CORE * Y,),
            in_specs=[field, field],
            out_specs=[
                pl.BlockSpec(block, lambda i, s: (jnp.minimum(i, Y - 1), 0, 0, 0)),
                pl.BlockSpec(block, lambda i, s: (jnp.maximum(i - Y, 0), 0, 0, 0)),
            ],
        ),
        out_shape=[
            jax.ShapeDtypeStruct((Y, step, rows, cols), BF16),
            jax.ShapeDtypeStruct((Y, step, rows, cols), F32),
        ],
        compiler_params=compiler_params(12),
        name="own_sum",
    )(start, spread, controls)


def chip_sum_kernel(keep_ref, arrived_ref, *outs):
    for d, out in enumerate(outs):
        for l in range(out.shape[0]):
            out[l] = (keep_ref[d, l] + arrived_ref[d, l].astype(F32)).astype(out.dtype)


def chip_sum(keep, arrived):
    vmem = pl.BlockSpec(memory_space=pltpu.VMEM)
    return pl.pallas_call(
        chip_sum_kernel,
        in_specs=[vmem] * 2,
        out_specs=[vmem] * Y,
        out_shape=[
            jax.ShapeDtypeStruct(keep.shape[1:], BF16 if d else F32) for d in range(Y)
        ],
        compiler_params=pltpu.CompilerParams(vmem_limit_bytes=8 * 1024 * 1024),
        name="chip_sum",
    )(keep, arrived)


def tables_kernel(me_ref, vert_ref, lon_ref, lat_ref, big_ref, lon_out_ref, turned_ref):
    me = me_ref[0]
    levels = vert_ref.shape[0]
    size = levels * 8
    row = lax.broadcasted_iota(jnp.int32, (size, levels), 0) >> 3
    col = lax.broadcasted_iota(jnp.int32, (size, levels), 1)
    source = (row & ~3) | ((row + 8 - me) & 3)
    pick_out = jnp.where(source == col, 1.0, 0.0).astype(BF16)
    pick_in = jnp.where(row == col, 1.0, 0.0).astype(BF16)
    tall = jnp.dot(pick_out, vert_ref[...], preferred_element_type=F32).astype(BF16)
    wide = nt_dot(tall, pick_in)
    r = lax.broadcasted_iota(jnp.int32, (size, size), 0) & 7
    c = lax.broadcasted_iota(jnp.int32, (size, size), 1) & 7
    big_ref[...] = jnp.where(r == c, wide, 0.0).astype(BF16)
    share = lon_ref.shape[0] // LATS
    for d in range(LATS):
        at = pl.multiple_of(((me + d) & (LATS - 1)) * share, share)
        lon_out_ref[share * d : share * d + share, :] = lon_ref[pl.ds(at, share), :]
    rows = lat_ref.shape[0]
    from_col = lax.broadcasted_iota(jnp.int32, (rows, rows), 0)
    to_col = lax.broadcasted_iota(jnp.int32, (rows, rows), 1)
    for turn in range(EACH):
        back = EACH * (to_col >> 7) + ((turn - (to_col >> 5)) & 3)
        want = (((me + 16 - back) & (LATS - 1)) << 5) | (to_col & 31)
        move = jnp.where(from_col == want, 1.0, 0.0).astype(BF16)
        turned_ref[turn] = jnp.dot(
            lat_ref[...], move, preferred_element_type=F32
        ).astype(BF16)


def tables(me, vert_loc, lon_loc, lat_loc):
    levels = vert_loc.shape[0]
    size = lat_loc.shape[0]
    return pl.pallas_call(
        tables_kernel,
        in_specs=[pl.BlockSpec(memory_space=pltpu.SMEM)]
        + [pl.BlockSpec(memory_space=pltpu.VMEM)] * 3,
        out_specs=[pl.BlockSpec(memory_space=pltpu.VMEM)] * 3,
        out_shape=[
            jax.ShapeDtypeStruct((levels * 8, levels * 8), BF16),
            jax.ShapeDtypeStruct(lon_loc.shape, BF16),
            jax.ShapeDtypeStruct((EACH, size, size), BF16),
        ],
        compiler_params=pltpu.CompilerParams(vmem_limit_bytes=16 * 1024 * 1024),
        cost_estimate=pl.CostEstimate(
            flops=600_000_000, bytes_accessed=2_000_000, transcendentals=0
        ),
        name="tables",
    )(me, vert_loc, lon_loc, lat_loc)


def join_kernel(*refs):
    *pieces, out_ref = refs
    for l in range(out_ref.shape[0]):
        total = pieces[0][l].astype(F32)
        for piece in pieces[1:]:
            total += piece[l].astype(F32)
        out_ref[l] = total.astype(BF16)


def join(pieces):
    vmem = pl.BlockSpec(memory_space=pltpu.VMEM)
    return pl.pallas_call(
        join_kernel,
        in_specs=[vmem] * len(pieces),
        out_specs=vmem,
        out_shape=jax.ShapeDtypeStruct(pieces[0].shape, BF16),
        compiler_params=pltpu.CompilerParams(vmem_limit_bytes=8 * 1024 * 1024),
        name="join",
    )(*pieces)


def weigh_kernel(first_ref, classes_ref, table_ref, *refs):
    *pieces, out_ref = refs
    classes = classes_ref[...]
    numbers = range(1, table_ref.shape[0])
    at = [classes == n for n in numbers]
    for l in range(out_ref.shape[0]):
        total = pieces[0][l].astype(F32)
        for piece in pieces[1:]:
            total += piece[l].astype(F32)
        precision = jnp.full(classes.shape, table_ref[0, first_ref[0] + l], F32)
        for n in numbers:
            precision = jnp.where(at[n - 1], table_ref[n, first_ref[0] + l], precision)
        out_ref[l] = (total * precision).astype(BF16)


def weigh(first, classes, prec_table, pieces):
    vmem = pl.BlockSpec(memory_space=pltpu.VMEM)
    smem = pl.BlockSpec(memory_space=pltpu.SMEM)
    return pl.pallas_call(
        weigh_kernel,
        in_specs=[smem, vmem, smem] + [vmem] * len(pieces),
        out_specs=vmem,
        out_shape=jax.ShapeDtypeStruct(pieces[0].shape, BF16),
        compiler_params=pltpu.CompilerParams(vmem_limit_bytes=8 * 1024 * 1024),
        name="weigh",
    )(first, classes, prec_table, *pieces)


def spread_out_kernel(start_ref, spread_ref, *refs):
    weights = refs[: CORE * Y]
    big_ref, lon_ref = refs[CORE * Y : CORE * Y + 2]
    outs = refs[CORE * Y + 2 : CORE * Y + 2 + LATS]
    adj, mixed = refs[CORE * Y + 2 + LATS :]
    levels, rows, cols = adj.shape
    step = levels // (CORE * Y)
    for n, piece in enumerate(weights):
        core = start_ref[0] ^ (n // Y)
        base = (core * Y + ((start_ref[1] - n % Y) & (Y - 1))) * step
        for i in range(step):
            adj[base + i] = spread_ref[0, base + i].astype(F32) * piece[i].astype(F32)
    for g in range(rows // 8):
        x = adj[:, 8 * g : 8 * g + 8, :].reshape(levels * 8, cols).astype(BF16)
        y = jnp.dot(big_ref[...], x, preferred_element_type=F32)
        mixed[:, 8 * g : 8 * g + 8, :] = y.reshape(levels, 8, cols)
    share = cols // LATS
    for n in range(levels * rows // 256):
        at = 256 // rows
        x = mixed[at * n : at * n + at].reshape(256, cols).astype(BF16)
        y = nt_dot(lon_ref[...], x).astype(BF16)
        for d, out in enumerate(outs):
            out[0, :, 256 * n : 256 * n + 256] = y[share * d : share * d + share]


def spread_out(start, spread, weights, big, lon, first, count):
    _, levels, rows, cols = spread.shape
    share = cols // LATS

    def whole(x):
        return pl.BlockSpec(x.shape, lambda k, s: (0,) * x.ndim)

    return pl.pallas_call(
        spread_out_kernel,
        grid_spec=pltpu.PrefetchScalarGridSpec(
            num_scalar_prefetch=1,
            grid=(count,),
            in_specs=[pl.BlockSpec((1, levels, rows, cols), lambda k, s: (first + k, 0, 0, 0))]
            + [whole(x) for x in (*weights, big, lon)],
            out_specs=[pl.BlockSpec((1, share, levels * rows), lambda k, s: (k, 0, 0))] * LATS,
            scratch_shapes=[pltpu.VMEM((levels, rows, cols), F32)] * 2,
        ),
        out_shape=[jax.ShapeDtypeStruct((count, share, levels * rows), BF16)] * LATS,
        compiler_params=compiler_params(24),
        cost_estimate=pl.CostEstimate(
            flops=count * 1_500_000_000, bytes_accessed=count * 2_500_000, transcendentals=0
        ),
        name="spread_out",
    )(start, spread, *weights, big, lon)


def finish_kernel(me_ref, *refs):
    parts = refs[:LATS]
    turned_ref, out_ref = refs[LATS], refs[-1]
    share = parts[0].shape[1]
    groups = parts[0].shape[2] // 128
    lane = lax.broadcasted_iota(jnp.int32, (share, 128), 1) >> 5
    at = [lane == q for q in range(3)]
    for turn in range(EACH):
        lines = []
        for g in range(groups):
            sides = []
            for part in range(2):
                tiles = [
                    parts[EACH * part + (turn - q) % EACH][0, :, 128 * g : 128 * g + 128]
                    for q in range(EACH)
                ]
                side = tiles[3]
                for q in range(3):
                    side = jnp.where(at[q], tiles[q], side)
                sides.append(side)
            lines.append(jnp.concatenate(sides, axis=1))
        x = jnp.concatenate(lines, axis=0)
        y = nt_dot(x, turned_ref[turn]).astype(BF16)
        level = (turn + 8 - me_ref[0]) & 3
        for g in range(groups):
            out_ref[0, EACH * g + level] = y[share * g : share * g + share]


def finish(me, parts, turned, first, members, so_far=None):
    count, share, wide = parts[0].shape
    size = turned.shape[1]
    levels = wide // 32
    args = (*parts, turned) if so_far is None else (*parts, turned, so_far)
    extra = [] if so_far is None else [pl.BlockSpec(memory_space=pl.ANY)]
    return pl.pallas_call(
        finish_kernel,
        grid_spec=pltpu.PrefetchScalarGridSpec(
            num_scalar_prefetch=1,
            grid=(count,),
            in_specs=[pl.BlockSpec((1, share, wide), lambda k, s: (k, 0, 0))] * LATS
            + [pl.BlockSpec(turned.shape, lambda k, s: (0, 0, 0))]
            + extra,
            out_specs=pl.BlockSpec((1, levels, share, size), lambda k, s: (first + k, 0, 0, 0)),
        ),
        out_shape=jax.ShapeDtypeStruct((members, levels, share, size), BF16),
        input_output_aliases={} if so_far is None else {len(args): 0},
        compiler_params=compiler_params(16),
        cost_estimate=pl.CostEstimate(
            flops=count * 700_000_000, bytes_accessed=count * 2_500_000, transcendentals=0
        ),
        name="finish",
    )(me, *args)


def passed_on(axis, pieces, order):
    count = len(pieces)
    parts = [pieces[0]] + [None] * (count - 1)
    for d in order:
        parts[d] = lax.ppermute(pieces[d], axis, [(i, (i + d) % count) for i in range(count)])
    return parts


def local(controls, spread, classes, prec_table, vert_loc, lon_loc, lat_loc):
    controls = pltpu.with_memory_space_constraint(controls, pltpu.HBM)
    spread = pltpu.with_memory_space_constraint(spread, pltpu.HBM)
    members, levels = spread.shape[:2]
    core, y = lax.axis_index("core"), lax.axis_index("y")
    here = jnp.stack([core, y])
    me = lax.axis_index(LAT).reshape(1)
    first = ((core * Y + y) * (levels // (CORE * Y))).reshape(1)
    swap = [(0, 1), (1, 0)]

    big, lon, turned = tables(me, vert_loc, lon_loc, lat_loc)
    send, keep = own_sum(spread, controls, here)
    pieces = chip_sum(keep, lax.ppermute(send, "core", swap))
    along_y = join(passed_on("y", pieces, range(1, Y)))
    along_z = passed_on("zh", [along_y] * ZH, range(1, ZH))
    weighted = weigh(first, classes, prec_table, along_z)
    own = passed_on("y", [weighted] * Y, range(1, Y))
    weights = own + [lax.ppermute(x, "core", swap) for x in own]

    result = None
    for start, count in GROUPS:
        sending = spread_out(here, spread, weights, big, lon, start, count)
        parts = passed_on(LAT, sending, ORDER)
        result = finish(me, parts, turned, start, members, result)
    return result


def solution(mesh):
    finer = Mesh(
        mesh.devices.reshape(ZH, Y, CORE, mesh.shape["lat"]), ("zh", "y", "core", LAT)
    )
    members = P(("zh", "y", "core"), None, LAT, None)
    return jax.shard_map(
        local,
        mesh=finer,
        in_specs=(members, members, P(LAT, None), P(), P(), P(), P()),
        out_specs=members,
        check_vma=False,
    )
```

```python
import functools

import jax
import jax.numpy as jnp
from jax import lax
from jax.experimental import pallas as pl
from jax.experimental.pallas import tpu as pltpu
from jax.sharding import Mesh
from jax.sharding import PartitionSpec as P


F32 = jnp.float32
BF16 = jnp.bfloat16
ZH, Y, CORE = 4, 4, 2
LATS = 8
LAT = "lat"
EACH = 4
GROUPS = ((0, 1), (1, 2), (3, 1))
ORDER = (6, 4, 2, 5, 7, 1, 3)


def nt_dot(a, b):
    return lax.dot_general(a, b, (((1,), (1,)), ((), ())), preferred_element_type=F32)


def half_sum_kernel(other, here_ref, spread_ref, controls_ref, out_ref, kept_ref, controls_buf, sems):
    step = out_ref.shape[1]
    copies = []
    for d in range(Y):
        at = ((here_ref[0] ^ other) * Y + ((here_ref[1] + d) & (Y - 1))) * step
        pair = (
            pltpu.make_async_copy(
                spread_ref.at[:, pl.ds(at, step)], kept_ref.at[d], sems.at[0, d]
            ),
            pltpu.make_async_copy(
                controls_ref.at[:, pl.ds(at, step)], controls_buf.at[d], sems.at[1, d]
            ),
        )
        for copy in pair:
            copy.start()
        copies.append(pair)
    for d, pair in enumerate(copies):
        for copy in pair:
            copy.wait()
        for l in range(step):
            total = kept_ref[d, 0, l].astype(F32) * controls_buf[d, 0, l].astype(F32)
            for k in range(1, kept_ref.shape[1]):
                total += kept_ref[d, k, l].astype(F32) * controls_buf[d, k, l].astype(F32)
            out_ref[d, l] = total.astype(out_ref.dtype)


def half_sum(other, here, spread, controls, dtype):
    members, levels, rows, cols = spread.shape
    step = levels // (CORE * Y)
    smem, vmem = (pl.BlockSpec(memory_space=space) for space in (pltpu.SMEM, pltpu.VMEM))
    hbm = pl.BlockSpec(memory_space=pltpu.HBM)
    field = (Y, members, step, rows, cols)
    return pl.pallas_call(
        functools.partial(half_sum_kernel, other),
        in_specs=[smem, hbm, hbm],
        out_specs=[vmem, vmem],
        out_shape=[
            jax.ShapeDtypeStruct((Y, step, rows, cols), dtype),
            jax.ShapeDtypeStruct(field, BF16),
        ],
        scratch_shapes=[pltpu.VMEM(field, BF16), pltpu.SemaphoreType.DMA((2, Y))],
        compiler_params=pltpu.CompilerParams(vmem_limit_bytes=12 * 1024 * 1024),
        cost_estimate=pl.CostEstimate(
            flops=300_000_000, bytes_accessed=4_200_000, transcendentals=0
        ),
    )(here, spread, controls)


def chip_sum_kernel(keep_ref, arrived_ref, *outs):
    for d, out in enumerate(outs):
        for l in range(out.shape[0]):
            out[l] = (keep_ref[d, l] + arrived_ref[d, l].astype(F32)).astype(out.dtype)


def chip_sum(keep, arrived):
    vmem = pl.BlockSpec(memory_space=pltpu.VMEM)
    return pl.pallas_call(
        chip_sum_kernel,
        in_specs=[vmem] * 2,
        out_specs=[vmem] * Y,
        out_shape=[
            jax.ShapeDtypeStruct(keep.shape[1:], BF16 if d else F32) for d in range(Y)
        ],
        compiler_params=pltpu.CompilerParams(vmem_limit_bytes=8 * 1024 * 1024),
        name="chip_sum",
    )(keep, arrived)


def tables_kernel(here_ref, vert_ref, lon_ref, lat_ref, big_ref, lon_out_ref, turned_ref):
    me = here_ref[2]
    levels = vert_ref.shape[0]
    size = levels * 8
    row = lax.broadcasted_iota(jnp.int32, (size, levels), 0) >> 3
    col = lax.broadcasted_iota(jnp.int32, (size, levels), 1)
    source = (row & ~3) | ((row + 8 - me) & 3)
    pick_out = jnp.where(source == col, 1.0, 0.0).astype(BF16)
    piece, step = row >> 3, levels // (CORE * Y)
    core = here_ref[0] ^ (piece >> 2)
    held = (core * Y + ((here_ref[1] + 8 - piece) & (Y - 1))) * step + (row & 7)
    pick_in = jnp.where(held == col, 1.0, 0.0).astype(BF16)
    tall = jnp.dot(pick_out, vert_ref[...], preferred_element_type=F32).astype(BF16)
    wide = nt_dot(tall, pick_in)
    r = lax.broadcasted_iota(jnp.int32, (size, size), 0) & 7
    c = lax.broadcasted_iota(jnp.int32, (size, size), 1) & 7
    big_ref[...] = jnp.where(r == c, wide, 0.0).astype(BF16)
    share = lon_ref.shape[0] // LATS
    for d in range(LATS):
        at = pl.multiple_of(((me + d) & (LATS - 1)) * share, share)
        lon_out_ref[share * d : share * d + share, :] = lon_ref[pl.ds(at, share), :]
    rows = lat_ref.shape[0]
    from_col = lax.broadcasted_iota(jnp.int32, (rows, rows), 0)
    to_col = lax.broadcasted_iota(jnp.int32, (rows, rows), 1)
    for turn in range(EACH):
        back = EACH * (to_col >> 7) + ((turn - (to_col >> 5)) & 3)
        want = (((me + 16 - back) & (LATS - 1)) << 5) | (to_col & 31)
        move = jnp.where(from_col == want, 1.0, 0.0).astype(BF16)
        turned_ref[turn] = jnp.dot(
            lat_ref[...], move, preferred_element_type=F32
        ).astype(BF16)


def tables(here, vert_loc, lon_loc, lat_loc):
    levels = vert_loc.shape[0]
    size = lat_loc.shape[0]
    return pl.pallas_call(
        tables_kernel,
        in_specs=[pl.BlockSpec(memory_space=pltpu.SMEM)]
        + [pl.BlockSpec(memory_space=pltpu.VMEM)] * 3,
        out_specs=[pl.BlockSpec(memory_space=pltpu.VMEM)] * 3,
        out_shape=[
            jax.ShapeDtypeStruct((levels * 8, levels * 8), BF16),
            jax.ShapeDtypeStruct(lon_loc.shape, BF16),
            jax.ShapeDtypeStruct((EACH, size, size), BF16),
        ],
        compiler_params=pltpu.CompilerParams(vmem_limit_bytes=16 * 1024 * 1024),
        cost_estimate=pl.CostEstimate(
            flops=600_000_000, bytes_accessed=2_000_000, transcendentals=0
        ),
        name="tables",
    )(here, vert_loc, lon_loc, lat_loc)


def join_kernel(*refs):
    *pieces, out_ref = refs
    for l in range(out_ref.shape[0]):
        total = pieces[0][l].astype(F32)
        for piece in pieces[1:]:
            total += piece[l].astype(F32)
        out_ref[l] = total.astype(BF16)


def join(pieces):
    vmem = pl.BlockSpec(memory_space=pltpu.VMEM)
    return pl.pallas_call(
        join_kernel,
        in_specs=[vmem] * len(pieces),
        out_specs=vmem,
        out_shape=jax.ShapeDtypeStruct(pieces[0].shape, BF16),
        compiler_params=pltpu.CompilerParams(vmem_limit_bytes=8 * 1024 * 1024),
        name="join",
    )(*pieces)


def weigh_kernel(here_ref, classes_ref, table_ref, *refs):
    *pieces, out_ref = refs
    classes = classes_ref[...]
    first = (here_ref[0] * Y + here_ref[1]) * out_ref.shape[0]
    numbers = range(1, table_ref.shape[0])
    at = [classes == n for n in numbers]
    for l in range(out_ref.shape[0]):
        total = pieces[0][l].astype(F32)
        for piece in pieces[1:]:
            total += piece[l].astype(F32)
        precision = jnp.full(classes.shape, table_ref[0, first + l], F32)
        for n in numbers:
            precision = jnp.where(at[n - 1], table_ref[n, first + l], precision)
        out_ref[l] = (total * precision).astype(BF16)


def weigh(here, classes, prec_table, pieces):
    vmem = pl.BlockSpec(memory_space=pltpu.VMEM)
    smem = pl.BlockSpec(memory_space=pltpu.SMEM)
    return pl.pallas_call(
        weigh_kernel,
        in_specs=[smem, vmem, smem] + [vmem] * len(pieces),
        out_specs=vmem,
        out_shape=jax.ShapeDtypeStruct(pieces[0].shape, BF16),
        compiler_params=pltpu.CompilerParams(vmem_limit_bytes=8 * 1024 * 1024),
        name="weigh",
    )(here, classes, prec_table, *pieces)


def spread_out_kernel(first, *refs):
    pieces = CORE * Y
    weights, kept, refs = refs[:pieces], refs[pieces : pieces + CORE], refs[pieces + CORE :]
    big_ref, lon_ref, outs = refs[0], refs[1], refs[2 : 2 + LATS]
    adj, mixed = refs[2 + LATS :]
    levels, rows, cols = adj.shape
    step = levels // pieces
    share = cols // LATS

    def member(k):
        for low in range(0, rows, 16):
            for n, piece in enumerate(weights):
                for i in range(step):
                    own = kept[n // Y][-n % Y, first + k, i, low : low + 16, :]
                    weight = piece[i, low : low + 16, :]
                    adj[n * step + i, low : low + 16, :] = own.astype(F32) * weight.astype(F32)
            for at in range(low, low + 16, 8):
                x = adj[:, at : at + 8, :].reshape(levels * 8, cols).astype(BF16)
                y = jnp.dot(big_ref[...], x, preferred_element_type=F32)
                mixed[:, at : at + 8, :] = y.reshape(levels, 8, cols)
        block = 256 // rows
        for n in range(levels // block):
            x = mixed[block * n : block * n + block].reshape(256, cols).astype(BF16)
            y = nt_dot(lon_ref[...], x).astype(BF16)
            for d, out in enumerate(outs):
                out[k, :, 256 * n : 256 * n + 256] = y[share * d : share * d + share]

    count = outs[0].shape[0]
    if count == 1:
        member(0)
    else:
        pl.loop(0, count)(member)


def spread_out(weights, kept, big, lon, first, count):
    levels = len(weights) * weights[0].shape[0]
    _, rows, cols = weights[0].shape
    share = cols // LATS
    vmem = pl.BlockSpec(memory_space=pltpu.VMEM)
    args = (*weights, *kept, big, lon)
    return pl.pallas_call(
        functools.partial(spread_out_kernel, first),
        in_specs=[vmem] * len(args),
        out_specs=[vmem] * LATS,
        out_shape=[jax.ShapeDtypeStruct((count, share, levels * rows), BF16)] * LATS,
        scratch_shapes=[pltpu.VMEM((levels, rows, cols), F32)] * 2,
        compiler_params=pltpu.CompilerParams(vmem_limit_bytes=24 * 1024 * 1024),
        cost_estimate=pl.CostEstimate(
            flops=count * 1_500_000_000, bytes_accessed=count * 2_500_000, transcendentals=0
        ),
        name="spread_out",
    )(*args)


def finish_kernel(here_ref, *refs):
    parts = refs[:LATS]
    turned_ref, out_ref = refs[LATS], refs[-1]
    k, h = pl.program_id(0), pl.program_id(1)
    share = parts[0].shape[1]
    groups = out_ref.shape[1] // EACH
    lane = lax.broadcasted_iota(jnp.int32, (share, 128), 1) >> 5
    at = [lane == q for q in range(3)]
    for turn in range(EACH):
        lines = []
        for g in range(groups):
            lanes = pl.ds(pl.multiple_of((h * groups + g) * 128, 128), 128)
            sides = []
            for part in range(2):
                tiles = [parts[EACH * part + (turn - q) % EACH][k, :, lanes] for q in range(EACH)]
                side = tiles[3]
                for q in range(3):
                    side = jnp.where(at[q], tiles[q], side)
                sides.append(side)
            lines.append(jnp.concatenate(sides, axis=1))
        x = jnp.concatenate(lines, axis=0)
        y = nt_dot(x, turned_ref[turn]).astype(BF16)
        level = (turn + 8 - here_ref[2]) & 3
        for g in range(groups):
            out_ref[0, EACH * g + level] = y[share * g : share * g + share]


def finish(here, parts, turned, first, members, so_far=None):
    count, share, wide = parts[0].shape
    size = turned.shape[1]
    levels = wide // 32
    args = (*parts, turned) if so_far is None else (*parts, turned, so_far)
    extra = [] if so_far is None else [pl.BlockSpec(memory_space=pl.ANY)]
    vmem = pl.BlockSpec(memory_space=pltpu.VMEM)
    return pl.pallas_call(
        finish_kernel,
        grid_spec=pltpu.PrefetchScalarGridSpec(
            num_scalar_prefetch=1,
            grid=(count, 2),
            in_specs=[vmem] * (LATS + 1) + extra,
            out_specs=pl.BlockSpec(
                (1, levels // 2, share, size), lambda k, h, s: (first + k, h, 0, 0)
            ),
        ),
        out_shape=jax.ShapeDtypeStruct((members, levels, share, size), BF16),
        input_output_aliases={} if so_far is None else {len(args): 0},
        compiler_params=pltpu.CompilerParams(
            dimension_semantics=("arbitrary", "arbitrary"), vmem_limit_bytes=16 * 1024 * 1024
        ),
        cost_estimate=pl.CostEstimate(
            flops=count * 700_000_000, bytes_accessed=count * 2_500_000, transcendentals=0
        ),
        name="finish",
    )(here, *args)


def passed_on(axis, pieces, order):
    count = len(pieces)
    parts = [pieces[0]] + [None] * (count - 1)
    for d in order:
        parts[d] = lax.ppermute(pieces[d], axis, [(i, (i + d) % count) for i in range(count)])
    return parts


def local(controls, spread, classes, prec_table, vert_loc, lon_loc, lat_loc):
    controls = pltpu.with_memory_space_constraint(controls, pltpu.HBM)
    spread = pltpu.with_memory_space_constraint(spread, pltpu.HBM)
    members = spread.shape[0]
    here = jnp.stack([lax.axis_index(name) for name in ("core", "y", LAT)])
    swap = [(0, 1), (1, 0)]

    big, lon, turned = tables(here, vert_loc, lon_loc, lat_loc)
    send, kept_other = half_sum(1, here, spread, controls, BF16)
    keep, kept_own = half_sum(0, here, spread, controls, F32)
    arrived = lax.ppermute(send, "core", swap)
    pieces = chip_sum(keep, arrived)
    along_y = join(passed_on("y", pieces, range(1, Y)))
    along_z = passed_on("zh", [along_y] * ZH, range(1, ZH))
    weighted = weigh(here, classes, prec_table, along_z)
    own = passed_on("y", [weighted] * Y, range(1, Y))
    weights = own + [lax.ppermute(x, "core", swap) for x in own]

    result = None
    for start, count in GROUPS:
        sending = spread_out(weights, (kept_own, kept_other), big, lon, start, count)
        parts = passed_on(LAT, sending, ORDER)
        result = finish(here, parts, turned, start, members, result)
    return result


def solution(mesh):
    finer = Mesh(
        mesh.devices.reshape(ZH, Y, CORE, mesh.shape["lat"]), ("zh", "y", "core", LAT)
    )
    members = P(("zh", "y", "core"), None, LAT, None)
    return jax.shard_map(
        local,
        mesh=finer,
        in_specs=(members, members, P(LAT, None), P(), P(), P(), P()),
        out_specs=members,
        check_vma=False,
    )
```

```python
import functools

import jax
import jax.numpy as jnp
from jax import lax
from jax.experimental import pallas as pl
from jax.experimental.pallas import tpu as pltpu
from jax.sharding import Mesh
from jax.sharding import PartitionSpec as P


F32 = jnp.float32
BF16 = jnp.bfloat16
ZH, Y, CORE = 4, 4, 2
LATS = 8
LAT = "lat"
EACH = 4
Z_ORDER = (2, 1, 3)
GROUPS = ((0, 1), (1, 2), (3, 1))
ORDER = (6, 4, 2, 5, 7, 1, 3)


def nt_dot(a, b):
    return lax.dot_general(a, b, (((1,), (1,)), ((), ())), preferred_element_type=F32)


def half_sum_kernel(other, here_ref, spread_ref, controls_ref, out_ref, kept_ref, controls_buf, sems):
    step = out_ref.shape[1]
    copies = []
    for d in range(Y):
        at = ((here_ref[0] ^ other) * Y + ((here_ref[1] + d) & (Y - 1))) * step
        pair = (
            pltpu.make_async_copy(
                spread_ref.at[:, pl.ds(at, step)], kept_ref.at[d], sems.at[0, d]
            ),
            pltpu.make_async_copy(
                controls_ref.at[:, pl.ds(at, step)], controls_buf.at[d], sems.at[1, d]
            ),
        )
        for copy in pair:
            copy.start()
        copies.append(pair)
    for d, pair in enumerate(copies):
        for copy in pair:
            copy.wait()
        for l in range(step):
            total = kept_ref[d, 0, l].astype(F32) * controls_buf[d, 0, l].astype(F32)
            for k in range(1, kept_ref.shape[1]):
                total += kept_ref[d, k, l].astype(F32) * controls_buf[d, k, l].astype(F32)
            out_ref[d, l] = total.astype(out_ref.dtype)


def half_sum(other, here, spread, controls, dtype):
    members, levels, rows, cols = spread.shape
    step = levels // (CORE * Y)
    smem, vmem = (pl.BlockSpec(memory_space=space) for space in (pltpu.SMEM, pltpu.VMEM))
    hbm = pl.BlockSpec(memory_space=pltpu.HBM)
    field = (Y, members, step, rows, cols)
    return pl.pallas_call(
        functools.partial(half_sum_kernel, other),
        in_specs=[smem, hbm, hbm],
        out_specs=[vmem, vmem],
        out_shape=[
            jax.ShapeDtypeStruct((Y, step, rows, cols), dtype),
            jax.ShapeDtypeStruct(field, BF16),
        ],
        scratch_shapes=[pltpu.VMEM(field, BF16), pltpu.SemaphoreType.DMA((2, Y))],
        compiler_params=pltpu.CompilerParams(vmem_limit_bytes=12 * 1024 * 1024),
        cost_estimate=pl.CostEstimate(
            flops=300_000_000, bytes_accessed=4_200_000, transcendentals=0
        ),
    )(here, spread, controls)


def chip_sum_kernel(keep_ref, arrived_ref, *outs):
    for d, out in enumerate(outs):
        for l in range(out.shape[0]):
            out[l] = (keep_ref[d, l] + arrived_ref[d, l].astype(F32)).astype(out.dtype)


def chip_sum(keep, arrived):
    vmem = pl.BlockSpec(memory_space=pltpu.VMEM)
    return pl.pallas_call(
        chip_sum_kernel,
        in_specs=[vmem] * 2,
        out_specs=[vmem] * Y,
        out_shape=[
            jax.ShapeDtypeStruct(keep.shape[1:], BF16 if d else F32) for d in range(Y)
        ],
        compiler_params=pltpu.CompilerParams(vmem_limit_bytes=8 * 1024 * 1024),
        name="chip_sum",
    )(keep, arrived)


def tables_kernel(here_ref, vert_ref, lon_ref, lat_ref, big_ref, lon_out_ref, turned_ref):
    me = here_ref[2]
    levels = vert_ref.shape[0]
    size = levels * 8
    row = lax.broadcasted_iota(jnp.int32, (size, levels), 0) >> 3
    col = lax.broadcasted_iota(jnp.int32, (size, levels), 1)
    source = (row & ~3) | ((row + 8 - me) & 3)
    pick_out = jnp.where(source == col, 1.0, 0.0).astype(BF16)
    piece, step = row >> 3, levels // (CORE * Y)
    core = here_ref[0] ^ (piece >> 2)
    held = (core * Y + ((here_ref[1] + 8 - piece) & (Y - 1))) * step + (row & 7)
    pick_in = jnp.where(held == col, 1.0, 0.0).astype(BF16)
    tall = jnp.dot(pick_out, vert_ref[...], preferred_element_type=F32).astype(BF16)
    wide = nt_dot(tall, pick_in)
    r = lax.broadcasted_iota(jnp.int32, (size, size), 0) & 7
    c = lax.broadcasted_iota(jnp.int32, (size, size), 1) & 7
    big_ref[...] = jnp.where(r == c, wide, 0.0).astype(BF16)
    share = lon_ref.shape[0] // LATS
    for d in range(LATS):
        at = pl.multiple_of(((me + d) & (LATS - 1)) * share, share)
        lon_out_ref[share * d : share * d + share, :] = lon_ref[pl.ds(at, share), :]
    rows = lat_ref.shape[0]
    from_col = lax.broadcasted_iota(jnp.int32, (rows, rows), 0)
    to_col = lax.broadcasted_iota(jnp.int32, (rows, rows), 1)
    for turn in range(EACH):
        back = EACH * (to_col >> 7) + ((turn - (to_col >> 5)) & 3)
        want = (((me + 16 - back) & (LATS - 1)) << 5) | (to_col & 31)
        move = jnp.where(from_col == want, 1.0, 0.0).astype(BF16)
        turned_ref[turn] = jnp.dot(
            lat_ref[...], move, preferred_element_type=F32
        ).astype(BF16)


def tables(here, vert_loc, lon_loc, lat_loc):
    levels = vert_loc.shape[0]
    size = lat_loc.shape[0]
    return pl.pallas_call(
        tables_kernel,
        in_specs=[pl.BlockSpec(memory_space=pltpu.SMEM)]
        + [pl.BlockSpec(memory_space=pltpu.VMEM)] * 3,
        out_specs=[pl.BlockSpec(memory_space=pltpu.VMEM)] * 3,
        out_shape=[
            jax.ShapeDtypeStruct((levels * 8, levels * 8), BF16),
            jax.ShapeDtypeStruct(lon_loc.shape, BF16),
            jax.ShapeDtypeStruct((EACH, size, size), BF16),
        ],
        compiler_params=pltpu.CompilerParams(vmem_limit_bytes=16 * 1024 * 1024),
        cost_estimate=pl.CostEstimate(
            flops=600_000_000, bytes_accessed=2_000_000, transcendentals=0
        ),
        name="tables",
    )(here, vert_loc, lon_loc, lat_loc)


def join_kernel(*refs):
    *pieces, out_ref = refs
    for l in range(out_ref.shape[0]):
        total = pieces[0][l].astype(F32)
        for piece in pieces[1:]:
            total += piece[l].astype(F32)
        out_ref[l] = total.astype(BF16)


def join(pieces):
    vmem = pl.BlockSpec(memory_space=pltpu.VMEM)
    return pl.pallas_call(
        join_kernel,
        in_specs=[vmem] * len(pieces),
        out_specs=vmem,
        out_shape=jax.ShapeDtypeStruct(pieces[0].shape, BF16),
        compiler_params=pltpu.CompilerParams(vmem_limit_bytes=8 * 1024 * 1024),
        name="join",
    )(*pieces)


def weigh_kernel(here_ref, classes_ref, table_ref, *refs):
    *pieces, out_ref = refs
    classes = classes_ref[...]
    first = (here_ref[0] * Y + here_ref[1]) * out_ref.shape[0]
    numbers = range(1, table_ref.shape[0])
    at = [classes == n for n in numbers]
    for l in range(out_ref.shape[0]):
        total = pieces[0][l].astype(F32)
        for piece in pieces[1:]:
            total += piece[l].astype(F32)
        precision = jnp.full(classes.shape, table_ref[0, first + l], F32)
        for n in numbers:
            precision = jnp.where(at[n - 1], table_ref[n, first + l], precision)
        out_ref[l] = (total * precision).astype(BF16)


def weigh(here, classes, prec_table, pieces):
    vmem = pl.BlockSpec(memory_space=pltpu.VMEM)
    smem = pl.BlockSpec(memory_space=pltpu.SMEM)
    return pl.pallas_call(
        weigh_kernel,
        in_specs=[smem, vmem, smem] + [vmem] * len(pieces),
        out_specs=vmem,
        out_shape=jax.ShapeDtypeStruct(pieces[0].shape, BF16),
        compiler_params=pltpu.CompilerParams(vmem_limit_bytes=8 * 1024 * 1024),
        name="weigh",
    )(here, classes, prec_table, *pieces)


def spread_out_kernel(first, *refs):
    pieces = CORE * Y
    weights, kept, refs = refs[:pieces], refs[pieces : pieces + CORE], refs[pieces + CORE :]
    big_ref, lon_ref, outs = refs[0], refs[1], refs[2 : 2 + LATS]
    adj, mixed = refs[2 + LATS :]
    levels, rows, cols = adj.shape
    step = levels // pieces
    share = cols // LATS

    def member(k):
        for low in range(0, rows, 16):
            for n, piece in enumerate(weights):
                for i in range(step):
                    own = kept[n // Y][-n % Y, first + k, i, low : low + 16, :]
                    weight = piece[i, low : low + 16, :]
                    adj[n * step + i, low : low + 16, :] = own.astype(F32) * weight.astype(F32)
            for at in range(low, low + 16, 8):
                x = adj[:, at : at + 8, :].reshape(levels * 8, cols).astype(BF16)
                y = jnp.dot(big_ref[...], x, preferred_element_type=F32)
                mixed[:, at : at + 8, :] = y.reshape(levels, 8, cols)
        block = 256 // rows
        for n in range(levels // block):
            x = mixed[block * n : block * n + block].reshape(256, cols).astype(BF16)
            y = nt_dot(lon_ref[...], x).astype(BF16)
            for d, out in enumerate(outs):
                out[k, :, 256 * n : 256 * n + 256] = y[share * d : share * d + share]

    count = outs[0].shape[0]
    if count == 1:
        member(0)
    else:
        pl.loop(0, count)(member)


def spread_out(weights, kept, big, lon, first, count):
    levels = len(weights) * weights[0].shape[0]
    _, rows, cols = weights[0].shape
    share = cols // LATS
    vmem = pl.BlockSpec(memory_space=pltpu.VMEM)
    args = (*weights, *kept, big, lon)
    return pl.pallas_call(
        functools.partial(spread_out_kernel, first),
        in_specs=[vmem] * len(args),
        out_specs=[vmem] * LATS,
        out_shape=[jax.ShapeDtypeStruct((count, share, levels * rows), BF16)] * LATS,
        scratch_shapes=[pltpu.VMEM((levels, rows, cols), F32)] * 2,
        compiler_params=pltpu.CompilerParams(vmem_limit_bytes=24 * 1024 * 1024),
        cost_estimate=pl.CostEstimate(
            flops=count * 1_500_000_000, bytes_accessed=count * 2_500_000, transcendentals=0
        ),
        name="spread_out",
    )(*args)


def finish_kernel(first, here_ref, *refs):
    parts, turned_ref = refs[:LATS], refs[LATS]
    out_ref, done, sems = refs[-3:]
    count, share, _ = parts[0].shape
    levels = done.shape[1]
    groups = levels // EACH // 2
    lane = lax.broadcasted_iota(jnp.int32, (share, 128), 1) >> 5
    at = [lane == q for q in range(3)]
    copies = []
    for k in range(count):
        for h in range(2):
            for turn in range(EACH):
                lines = []
                for g in range(h * groups, h * groups + groups):
                    sides = []
                    for part in range(2):
                        tiles = [
                            parts[EACH * part + (turn - q) % EACH][k, :, 128 * g : 128 * g + 128]
                            for q in range(EACH)
                        ]
                        side = tiles[3]
                        for q in range(3):
                            side = jnp.where(at[q], tiles[q], side)
                        sides.append(side)
                    lines.append(jnp.concatenate(sides, axis=1))
                x = jnp.concatenate(lines, axis=0)
                y = nt_dot(x, turned_ref[turn]).astype(BF16)
                level = (turn + 8 - here_ref[2]) & 3
                for g in range(groups):
                    done[k, EACH * (h * groups + g) + level] = y[share * g : share * g + share]
            half = pl.ds(h * (levels // 2), levels // 2)
            copy = pltpu.make_async_copy(
                done.at[k, half], out_ref.at[first + k, half], sems.at[k, h]
            )
            copy.start()
            copies.append(copy)
    for copy in copies:
        copy.wait()


def finish(here, parts, turned, first, members, so_far=None):
    count, share, wide = parts[0].shape
    size = turned.shape[1]
    levels = wide // 32
    args = (here, *parts, turned)
    smem, vmem = (pl.BlockSpec(memory_space=space) for space in (pltpu.SMEM, pltpu.VMEM))
    hbm = pl.BlockSpec(memory_space=pltpu.HBM)
    in_specs = [smem] + [vmem] * (LATS + 1)
    aliases = {}
    if so_far is not None:
        aliases = {len(args): 0}
        args, in_specs = (*args, so_far), in_specs + [hbm]
    return pl.pallas_call(
        functools.partial(finish_kernel, first),
        in_specs=in_specs,
        out_specs=hbm,
        out_shape=jax.ShapeDtypeStruct((members, levels, share, size), BF16),
        input_output_aliases=aliases,
        scratch_shapes=[
            pltpu.VMEM((count, levels, share, size), BF16),
            pltpu.SemaphoreType.DMA((count, 2)),
        ],
        compiler_params=pltpu.CompilerParams(vmem_limit_bytes=16 * 1024 * 1024),
        cost_estimate=pl.CostEstimate(
            flops=count * 700_000_000, bytes_accessed=count * 2_500_000, transcendentals=0
        ),
        name="finish",
    )(*args)


def passed_on(axis, pieces, order):
    count = len(pieces)
    parts = [pieces[0]] + [None] * (count - 1)
    for d in order:
        parts[d] = lax.ppermute(pieces[d], axis, [(i, (i + d) % count) for i in range(count)])
    return parts


def local(controls, spread, classes, prec_table, vert_loc, lon_loc, lat_loc):
    controls = pltpu.with_memory_space_constraint(controls, pltpu.HBM)
    spread = pltpu.with_memory_space_constraint(spread, pltpu.HBM)
    members = spread.shape[0]
    here = jnp.stack([lax.axis_index(name) for name in ("core", "y", LAT)])
    swap = [(0, 1), (1, 0)]

    big, lon, turned = tables(here, vert_loc, lon_loc, lat_loc)
    send, kept_other = half_sum(1, here, spread, controls, BF16)
    keep, kept_own = half_sum(0, here, spread, controls, F32)
    arrived = lax.ppermute(send, "core", swap)
    pieces = chip_sum(keep, arrived)
    along_y = join(passed_on("y", pieces, range(1, Y)))
    along_z = passed_on("zh", [along_y] * ZH, Z_ORDER)
    weighted = weigh(here, classes, prec_table, along_z)
    own = passed_on("y", [weighted] * Y, range(1, Y))
    weights = own + [lax.ppermute(x, "core", swap) for x in own]

    result = None
    for start, count in GROUPS:
        sending = spread_out(weights, (kept_own, kept_other), big, lon, start, count)
        parts = passed_on(LAT, sending, ORDER)
        result = finish(here, parts, turned, start, members, result)
    return result


def solution(mesh):
    finer = Mesh(
        mesh.devices.reshape(ZH, Y, CORE, mesh.shape["lat"]), ("zh", "y", "core", LAT)
    )
    members = P(("zh", "y", "core"), None, LAT, None)
    return jax.shard_map(
        local,
        mesh=finer,
        in_specs=(members, members, P(LAT, None), P(), P(), P(), P()),
        out_specs=members,
        check_vma=False,
    )
```

```python
import functools

import jax
import jax.numpy as jnp
from jax import lax
from jax.experimental import pallas as pl
from jax.experimental.pallas import tpu as pltpu
from jax.sharding import Mesh
from jax.sharding import PartitionSpec as P


F32 = jnp.float32
BF16 = jnp.bfloat16
ZH, Y, CORE = 4, 4, 2
LATS = 8
LAT = "lat"
EACH = 4
Z_ORDER = (2, 1, 3)
GROUPS = ((0, 1), (1, 2), (3, 1))
ORDER = (6, 4, 2, 5, 7, 1, 3)


def nt_dot(a, b):
    return lax.dot_general(a, b, (((1,), (1,)), ((), ())), preferred_element_type=F32)


def other_half_kernel(here_ref, spread_ref, controls_ref, out_ref, kept_ref, own_ref, buf, sems):
    step = out_ref.shape[1]
    copies = []
    for other in (1, 0):
        for d in range(Y):
            at = ((here_ref[0] ^ other) * Y + ((here_ref[1] + d) & (Y - 1))) * step
            target = buf if other else own_ref
            pair = (
                pltpu.make_async_copy(
                    spread_ref.at[:, pl.ds(at, step)], kept_ref.at[other, d], sems.at[0, other, d]
                ),
                pltpu.make_async_copy(
                    controls_ref.at[:, pl.ds(at, step)], target.at[d], sems.at[1, other, d]
                ),
            )
            for copy in pair:
                copy.start()
            copies.append(pair)
    for n, pair in enumerate(copies):
        for copy in pair:
            copy.wait()
        if n < Y:
            add_members(kept_ref.at[1, n], buf.at[n], out_ref.at[n])


def add_members(spread_ref, controls_ref, out_ref):
    for l in range(out_ref.shape[0]):
        total = spread_ref[0, l].astype(F32) * controls_ref[0, l].astype(F32)
        for k in range(1, spread_ref.shape[0]):
            total += spread_ref[k, l].astype(F32) * controls_ref[k, l].astype(F32)
        out_ref[l] = total.astype(out_ref.dtype)


def other_half(here, spread, controls):
    members, levels, rows, cols = spread.shape
    step = levels // (CORE * Y)
    smem, vmem = (pl.BlockSpec(memory_space=space) for space in (pltpu.SMEM, pltpu.VMEM))
    hbm = pl.BlockSpec(memory_space=pltpu.HBM)
    field = (Y, members, step, rows, cols)
    return pl.pallas_call(
        other_half_kernel,
        in_specs=[smem, hbm, hbm],
        out_specs=[vmem] * 3,
        out_shape=[
            jax.ShapeDtypeStruct((Y, step, rows, cols), BF16),
            jax.ShapeDtypeStruct((CORE, *field), BF16),
            jax.ShapeDtypeStruct(field, BF16),
        ],
        scratch_shapes=[pltpu.VMEM(field, BF16), pltpu.SemaphoreType.DMA((2, CORE, Y))],
        compiler_params=pltpu.CompilerParams(vmem_limit_bytes=12 * 1024 * 1024),
        name="other_half",
    )(here, spread, controls)


def own_half_kernel(kept_ref, controls_ref, out_ref):
    for d in range(Y):
        add_members(kept_ref.at[0, d], controls_ref.at[d], out_ref.at[d])


def own_half(kept, controls):
    _, _, _, step, rows, cols = kept.shape
    vmem = pl.BlockSpec(memory_space=pltpu.VMEM)
    return pl.pallas_call(
        own_half_kernel,
        in_specs=[vmem] * 2,
        out_specs=vmem,
        out_shape=jax.ShapeDtypeStruct((Y, step, rows, cols), F32),
        compiler_params=pltpu.CompilerParams(vmem_limit_bytes=12 * 1024 * 1024),
        cost_estimate=pl.CostEstimate(
            flops=300_000_000, bytes_accessed=4_200_000, transcendentals=0
        ),
        name="own_half",
    )(kept, controls)


def chip_sum_kernel(keep_ref, arrived_ref, *outs):
    for d, out in enumerate(outs):
        for l in range(out.shape[0]):
            out[l] = (keep_ref[d, l] + arrived_ref[d, l].astype(F32)).astype(out.dtype)


def chip_sum(keep, arrived):
    vmem = pl.BlockSpec(memory_space=pltpu.VMEM)
    return pl.pallas_call(
        chip_sum_kernel,
        in_specs=[vmem] * 2,
        out_specs=[vmem] * Y,
        out_shape=[
            jax.ShapeDtypeStruct(keep.shape[1:], BF16 if d else F32) for d in range(Y)
        ],
        compiler_params=pltpu.CompilerParams(vmem_limit_bytes=8 * 1024 * 1024),
        name="chip_sum",
    )(keep, arrived)


def tables_kernel(
    here_ref, table_ref, classes_ref, vert_ref, lon_ref, lat_ref,
    precision_ref, big_ref, lon_out_ref, turned_ref,
):
    classes = classes_ref[...]
    numbers = range(1, table_ref.shape[0])
    is_class = [classes == n for n in numbers]
    count = precision_ref.shape[0]
    first = (here_ref[0] * Y + here_ref[1]) * count
    for l in range(count):
        precision = jnp.full(classes.shape, table_ref[0, first + l], F32)
        for n in numbers:
            precision = jnp.where(is_class[n - 1], table_ref[n, first + l], precision)
        precision_ref[l] = precision
    me = here_ref[2]
    levels = vert_ref.shape[0]
    size = levels * 8
    row = lax.broadcasted_iota(jnp.int32, (size, levels), 0) >> 3
    col = lax.broadcasted_iota(jnp.int32, (size, levels), 1)
    source = (row & ~3) | ((row + 8 - me) & 3)
    pick_out = jnp.where(source == col, 1.0, 0.0).astype(BF16)
    piece, step = row >> 3, levels // (CORE * Y)
    core = here_ref[0] ^ (piece >> 2)
    held = (core * Y + ((here_ref[1] + 8 - piece) & (Y - 1))) * step + (row & 7)
    pick_in = jnp.where(held == col, 1.0, 0.0).astype(BF16)
    tall = jnp.dot(pick_out, vert_ref[...], preferred_element_type=F32).astype(BF16)
    wide = nt_dot(tall, pick_in)
    r = lax.broadcasted_iota(jnp.int32, (size, size), 0) & 7
    c = lax.broadcasted_iota(jnp.int32, (size, size), 1) & 7
    big_ref[...] = jnp.where(r == c, wide, 0.0).astype(BF16)
    share = lon_ref.shape[0] // LATS
    for d in range(LATS):
        at = pl.multiple_of(((me + d) & (LATS - 1)) * share, share)
        lon_out_ref[share * d : share * d + share, :] = lon_ref[pl.ds(at, share), :]
    rows = lat_ref.shape[0]
    from_col = lax.broadcasted_iota(jnp.int32, (rows, rows), 0)
    to_col = lax.broadcasted_iota(jnp.int32, (rows, rows), 1)
    for turn in range(EACH):
        back = EACH * (to_col >> 7) + ((turn - (to_col >> 5)) & 3)
        want = (((me + 16 - back) & (LATS - 1)) << 5) | (to_col & 31)
        move = jnp.where(from_col == want, 1.0, 0.0).astype(BF16)
        turned_ref[turn] = jnp.dot(
            lat_ref[...], move, preferred_element_type=F32
        ).astype(BF16)


def tables(here, prec_table, classes, vert_loc, lon_loc, lat_loc):
    levels = vert_loc.shape[0]
    size = lat_loc.shape[0]
    return pl.pallas_call(
        tables_kernel,
        in_specs=[pl.BlockSpec(memory_space=pltpu.SMEM)] * 2
        + [pl.BlockSpec(memory_space=pltpu.VMEM)] * 4,
        out_specs=[pl.BlockSpec(memory_space=pltpu.VMEM)] * 4,
        out_shape=[
            jax.ShapeDtypeStruct((levels // (CORE * Y), *classes.shape), F32),
            jax.ShapeDtypeStruct((levels * 8, levels * 8), BF16),
            jax.ShapeDtypeStruct(lon_loc.shape, BF16),
            jax.ShapeDtypeStruct((EACH, size, size), BF16),
        ],
        compiler_params=pltpu.CompilerParams(vmem_limit_bytes=16 * 1024 * 1024),
        cost_estimate=pl.CostEstimate(
            flops=600_000_000, bytes_accessed=2_000_000, transcendentals=0
        ),
        name="tables",
    )(here, prec_table, classes, vert_loc, lon_loc, lat_loc)


def join_kernel(*refs):
    *pieces, out_ref = refs
    for l in range(out_ref.shape[0]):
        total = pieces[0][l].astype(F32)
        for piece in pieces[1:]:
            total += piece[l].astype(F32)
        out_ref[l] = total.astype(BF16)


def join(pieces):
    vmem = pl.BlockSpec(memory_space=pltpu.VMEM)
    return pl.pallas_call(
        join_kernel,
        in_specs=[vmem] * len(pieces),
        out_specs=vmem,
        out_shape=jax.ShapeDtypeStruct(pieces[0].shape, BF16),
        compiler_params=pltpu.CompilerParams(vmem_limit_bytes=8 * 1024 * 1024),
        name="join",
    )(*pieces)


def weigh_kernel(precision_ref, *refs):
    *pieces, out_ref = refs
    for l in range(out_ref.shape[0]):
        total = pieces[0][l].astype(F32)
        for piece in pieces[1:]:
            total += piece[l].astype(F32)
        out_ref[l] = (total * precision_ref[l]).astype(BF16)


def weigh(precision, pieces):
    vmem = pl.BlockSpec(memory_space=pltpu.VMEM)
    return pl.pallas_call(
        weigh_kernel,
        in_specs=[vmem] * (1 + len(pieces)),
        out_specs=vmem,
        out_shape=jax.ShapeDtypeStruct(pieces[0].shape, BF16),
        compiler_params=pltpu.CompilerParams(vmem_limit_bytes=8 * 1024 * 1024),
        name="weigh",
    )(precision, *pieces)


def spread_out_kernel(first, *refs):
    pieces = CORE * Y
    weights, kept, refs = refs[:pieces], refs[pieces], refs[pieces + 1 :]
    big_ref, lon_ref, outs = refs[0], refs[1], refs[2 : 2 + LATS]
    adj, mixed = refs[2 + LATS :]
    levels, rows, cols = adj.shape
    step = levels // pieces
    share = cols // LATS

    def member(k):
        for low in range(0, rows, 16):
            for n, piece in enumerate(weights):
                for i in range(step):
                    own = kept[n // Y, -n % Y, first + k, i, low : low + 16, :]
                    weight = piece[i, low : low + 16, :]
                    adj[n * step + i, low : low + 16, :] = own.astype(F32) * weight.astype(F32)
            for at in range(low, low + 16, 8):
                x = adj[:, at : at + 8, :].reshape(levels * 8, cols).astype(BF16)
                y = jnp.dot(big_ref[...], x, preferred_element_type=F32)
                mixed[:, at : at + 8, :] = y.reshape(levels, 8, cols)
        block = 256 // rows
        for n in range(levels // block):
            x = mixed[block * n : block * n + block].reshape(256, cols).astype(BF16)
            y = nt_dot(lon_ref[...], x).astype(BF16)
            for d, out in enumerate(outs):
                out[k, :, 256 * n : 256 * n + 256] = y[share * d : share * d + share]

    count = outs[0].shape[0]
    if count == 1:
        member(0)
    else:
        pl.loop(0, count)(member)


def spread_out(weights, kept, big, lon, first, count):
    levels = len(weights) * weights[0].shape[0]
    _, rows, cols = weights[0].shape
    share = cols // LATS
    vmem = pl.BlockSpec(memory_space=pltpu.VMEM)
    args = (*weights, kept, big, lon)
    return pl.pallas_call(
        functools.partial(spread_out_kernel, first),
        in_specs=[vmem] * len(args),
        out_specs=[vmem] * LATS,
        out_shape=[jax.ShapeDtypeStruct((count, share, levels * rows), BF16)] * LATS,
        scratch_shapes=[pltpu.VMEM((levels, rows, cols), F32)] * 2,
        compiler_params=pltpu.CompilerParams(vmem_limit_bytes=24 * 1024 * 1024),
        cost_estimate=pl.CostEstimate(
            flops=count * 1_500_000_000, bytes_accessed=count * 2_500_000, transcendentals=0
        ),
        name="spread_out",
    )(*args)


def finish_kernel(first, here_ref, *refs):
    parts, turned_ref = refs[:LATS], refs[LATS]
    out_ref, done, sems = refs[-3:]
    count, share, _ = parts[0].shape
    levels = done.shape[1]
    groups = levels // EACH // 2
    lane = lax.broadcasted_iota(jnp.int32, (share, 128), 1) >> 5
    at = [lane == q for q in range(3)]
    copies = []
    for k in range(count):
        for h in range(2):
            for turn in range(EACH):
                lines = []
                for g in range(h * groups, h * groups + groups):
                    sides = []
                    for part in range(2):
                        tiles = [
                            parts[EACH * part + (turn - q) % EACH][k, :, 128 * g : 128 * g + 128]
                            for q in range(EACH)
                        ]
                        side = tiles[3]
                        for q in range(3):
                            side = jnp.where(at[q], tiles[q], side)
                        sides.append(side)
                    lines.append(jnp.concatenate(sides, axis=1))
                x = jnp.concatenate(lines, axis=0)
                y = nt_dot(x, turned_ref[turn]).astype(BF16)
                level = (turn + 8 - here_ref[2]) & 3
                for g in range(groups):
                    done[k, EACH * (h * groups + g) + level] = y[share * g : share * g + share]
            half = pl.ds(h * (levels // 2), levels // 2)
            copy = pltpu.make_async_copy(
                done.at[k, half], out_ref.at[first + k, half], sems.at[k, h]
            )
            copy.start()
            copies.append(copy)
    for copy in copies:
        copy.wait()


def finish(here, parts, turned, first, members, so_far=None):
    count, share, wide = parts[0].shape
    size = turned.shape[1]
    levels = wide // 32
    args = (here, *parts, turned)
    smem, vmem = (pl.BlockSpec(memory_space=space) for space in (pltpu.SMEM, pltpu.VMEM))
    hbm = pl.BlockSpec(memory_space=pltpu.HBM)
    in_specs = [smem] + [vmem] * (LATS + 1)
    aliases = {}
    if so_far is not None:
        aliases = {len(args): 0}
        args, in_specs = (*args, so_far), in_specs + [hbm]
    return pl.pallas_call(
        functools.partial(finish_kernel, first),
        in_specs=in_specs,
        out_specs=hbm,
        out_shape=jax.ShapeDtypeStruct((members, levels, share, size), BF16),
        input_output_aliases=aliases,
        scratch_shapes=[
            pltpu.VMEM((count, levels, share, size), BF16),
            pltpu.SemaphoreType.DMA((count, 2)),
        ],
        compiler_params=pltpu.CompilerParams(vmem_limit_bytes=16 * 1024 * 1024),
        cost_estimate=pl.CostEstimate(
            flops=count * 700_000_000, bytes_accessed=count * 2_500_000, transcendentals=0
        ),
        name="finish",
    )(*args)


def passed_on(axis, pieces, order):
    count = len(pieces)
    parts = [pieces[0]] + [None] * (count - 1)
    for d in order:
        parts[d] = lax.ppermute(pieces[d], axis, [(i, (i + d) % count) for i in range(count)])
    return parts


def local(controls, spread, classes, prec_table, vert_loc, lon_loc, lat_loc):
    controls = pltpu.with_memory_space_constraint(controls, pltpu.HBM)
    spread = pltpu.with_memory_space_constraint(spread, pltpu.HBM)
    members = spread.shape[0]
    here = jnp.stack([lax.axis_index(name) for name in ("core", "y", LAT)])
    swap = [(0, 1), (1, 0)]

    precision, big, lon, turned = tables(here, prec_table, classes, vert_loc, lon_loc, lat_loc)
    send, kept, own_controls = other_half(here, spread, controls)
    keep = own_half(kept, own_controls)
    arrived = lax.ppermute(send, "core", swap)
    pieces = chip_sum(keep, arrived)
    along_y = join(passed_on("y", pieces, range(1, Y)))
    along_z = passed_on("zh", [along_y] * ZH, Z_ORDER)
    weighted = weigh(precision, along_z)
    own = passed_on("y", [weighted] * Y, range(1, Y))
    weights = list(own)
    for x in own:
        weights.append(lax.ppermute(x, "core", swap))

    result = None
    for start, count in GROUPS:
        sending = spread_out(weights, kept, big, lon, start, count)
        parts = passed_on(LAT, sending, ORDER)
        result = finish(here, parts, turned, start, members, result)
    return result


def solution(mesh):
    finer = Mesh(
        mesh.devices.reshape(ZH, Y, CORE, mesh.shape["lat"]), ("zh", "y", "core", LAT)
    )
    members = P(("zh", "y", "core"), None, LAT, None)
    return jax.shard_map(
        local,
        mesh=finer,
        in_specs=(members, members, P(LAT, None), P(), P(), P(), P()),
        out_specs=members,
        check_vma=False,
    )
```

```python
import functools

import jax
import jax.numpy as jnp
from jax import lax
from jax.experimental import pallas as pl
from jax.experimental.pallas import tpu as pltpu
from jax.sharding import Mesh
from jax.sharding import PartitionSpec as P


F32 = jnp.float32
BF16 = jnp.bfloat16
ZH, Y, CORE = 4, 4, 2
LATS = 8
LAT = "lat"
EACH = 4
Z_ORDER = (2, 1, 3)
GROUPS = ((0, 2), (2, 2))
ORDER = (6, 4, 2, 5, 7, 1, 3)


def nt_dot(a, b):
    return lax.dot_general(a, b, (((1,), (1,)), ((), ())), preferred_element_type=F32)


def other_half_kernel(here_ref, spread_ref, controls_ref, out_ref, kept_ref, own_ref, buf, sems):
    step = out_ref.shape[1]
    copies = []
    for other in (1, 0):
        for d in range(Y):
            at = ((here_ref[0] ^ other) * Y + ((here_ref[1] + d) & (Y - 1))) * step
            target = buf if other else own_ref
            pair = (
                pltpu.make_async_copy(
                    spread_ref.at[:, pl.ds(at, step)], kept_ref.at[other, d], sems.at[0, other, d]
                ),
                pltpu.make_async_copy(
                    controls_ref.at[:, pl.ds(at, step)], target.at[d], sems.at[1, other, d]
                ),
            )
            for copy in pair:
                copy.start()
            copies.append(pair)
    for n, pair in enumerate(copies):
        for copy in pair:
            copy.wait()
        if n < Y:
            add_members(kept_ref.at[1, n], buf.at[n], out_ref.at[n])


def add_members(spread_ref, controls_ref, out_ref):
    for l in range(out_ref.shape[0]):
        total = spread_ref[0, l].astype(F32) * controls_ref[0, l].astype(F32)
        for k in range(1, spread_ref.shape[0]):
            total += spread_ref[k, l].astype(F32) * controls_ref[k, l].astype(F32)
        out_ref[l] = total.astype(out_ref.dtype)


def other_half(here, spread, controls):
    members, levels, rows, cols = spread.shape
    step = levels // (CORE * Y)
    smem, vmem = (pl.BlockSpec(memory_space=space) for space in (pltpu.SMEM, pltpu.VMEM))
    hbm = pl.BlockSpec(memory_space=pltpu.HBM)
    field = (Y, members, step, rows, cols)
    return pl.pallas_call(
        other_half_kernel,
        in_specs=[smem, hbm, hbm],
        out_specs=[vmem] * 3,
        out_shape=[
            jax.ShapeDtypeStruct((Y, step, rows, cols), BF16),
            jax.ShapeDtypeStruct((CORE, *field), BF16),
            jax.ShapeDtypeStruct(field, BF16),
        ],
        scratch_shapes=[pltpu.VMEM(field, BF16), pltpu.SemaphoreType.DMA((2, CORE, Y))],
        compiler_params=pltpu.CompilerParams(vmem_limit_bytes=12 * 1024 * 1024),
        name="other_half",
    )(here, spread, controls)


def own_half_kernel(kept_ref, controls_ref, out_ref):
    for d in range(Y):
        add_members(kept_ref.at[0, d], controls_ref.at[d], out_ref.at[d])


def own_half(kept, controls):
    _, _, _, step, rows, cols = kept.shape
    vmem = pl.BlockSpec(memory_space=pltpu.VMEM)
    return pl.pallas_call(
        own_half_kernel,
        in_specs=[vmem] * 2,
        out_specs=vmem,
        out_shape=jax.ShapeDtypeStruct((Y, step, rows, cols), F32),
        compiler_params=pltpu.CompilerParams(vmem_limit_bytes=12 * 1024 * 1024),
        cost_estimate=pl.CostEstimate(
            flops=300_000_000, bytes_accessed=4_200_000, transcendentals=0
        ),
        name="own_half",
    )(kept, controls)


def chip_sum_kernel(keep_ref, arrived_ref, *outs):
    for d, out in enumerate(outs):
        for l in range(out.shape[0]):
            out[l] = (keep_ref[d, l] + arrived_ref[d, l].astype(F32)).astype(out.dtype)


def chip_sum(keep, arrived):
    vmem = pl.BlockSpec(memory_space=pltpu.VMEM)
    return pl.pallas_call(
        chip_sum_kernel,
        in_specs=[vmem] * 2,
        out_specs=[vmem] * Y,
        out_shape=[
            jax.ShapeDtypeStruct(keep.shape[1:], BF16 if d else F32) for d in range(Y)
        ],
        compiler_params=pltpu.CompilerParams(vmem_limit_bytes=8 * 1024 * 1024),
        name="chip_sum",
    )(keep, arrived)


def tables_kernel(
    here_ref, table_ref, classes_ref, vert_ref, lon_ref, lat_ref,
    precision_ref, big_ref, lon_out_ref, turned_ref,
):
    classes = classes_ref[...]
    numbers = range(1, table_ref.shape[0])
    is_class = [classes == n for n in numbers]
    count = precision_ref.shape[0]
    first = (here_ref[0] * Y + here_ref[1]) * count
    for l in range(count):
        precision = jnp.full(classes.shape, table_ref[0, first + l], F32)
        for n in numbers:
            precision = jnp.where(is_class[n - 1], table_ref[n, first + l], precision)
        precision_ref[l] = precision
    me = here_ref[2]
    levels = vert_ref.shape[0]
    size = levels * 8
    row = lax.broadcasted_iota(jnp.int32, (size, levels), 0) >> 3
    col = lax.broadcasted_iota(jnp.int32, (size, levels), 1)
    source = (row & ~3) | ((row + 8 - me) & 3)
    pick_out = jnp.where(source == col, 1.0, 0.0).astype(BF16)
    piece, step = row >> 3, levels // (CORE * Y)
    core = here_ref[0] ^ (piece >> 2)
    held = (core * Y + ((here_ref[1] + 8 - piece) & (Y - 1))) * step + (row & 7)
    pick_in = jnp.where(held == col, 1.0, 0.0).astype(BF16)
    tall = jnp.dot(pick_out, vert_ref[...], preferred_element_type=F32).astype(BF16)
    wide = nt_dot(tall, pick_in)
    r = lax.broadcasted_iota(jnp.int32, (size, size), 0) & 7
    c = lax.broadcasted_iota(jnp.int32, (size, size), 1) & 7
    big_ref[...] = jnp.where(r == c, wide, 0.0).astype(BF16)
    share = lon_ref.shape[0] // LATS
    for d in range(LATS):
        at = pl.multiple_of(((me + d) & (LATS - 1)) * share, share)
        lon_out_ref[share * d : share * d + share, :] = lon_ref[pl.ds(at, share), :]
    rows = lat_ref.shape[0]
    from_col = lax.broadcasted_iota(jnp.int32, (rows, rows), 0)
    to_col = lax.broadcasted_iota(jnp.int32, (rows, rows), 1)
    for turn in range(EACH):
        back = EACH * (to_col >> 7) + ((turn - (to_col >> 5)) & 3)
        want = (((me + 16 - back) & (LATS - 1)) << 5) | (to_col & 31)
        move = jnp.where(from_col == want, 1.0, 0.0).astype(BF16)
        turned_ref[turn] = jnp.dot(
            lat_ref[...], move, preferred_element_type=F32
        ).astype(BF16)


def tables(here, prec_table, classes, vert_loc, lon_loc, lat_loc):
    levels = vert_loc.shape[0]
    size = lat_loc.shape[0]
    return pl.pallas_call(
        tables_kernel,
        in_specs=[pl.BlockSpec(memory_space=pltpu.SMEM)] * 2
        + [pl.BlockSpec(memory_space=pltpu.VMEM)] * 4,
        out_specs=[pl.BlockSpec(memory_space=pltpu.VMEM)] * 4,
        out_shape=[
            jax.ShapeDtypeStruct((levels // (CORE * Y), *classes.shape), F32),
            jax.ShapeDtypeStruct((levels * 8, levels * 8), BF16),
            jax.ShapeDtypeStruct(lon_loc.shape, BF16),
            jax.ShapeDtypeStruct((EACH, size, size), BF16),
        ],
        compiler_params=pltpu.CompilerParams(vmem_limit_bytes=16 * 1024 * 1024),
        cost_estimate=pl.CostEstimate(
            flops=600_000_000, bytes_accessed=2_000_000, transcendentals=0
        ),
        name="tables",
    )(here, prec_table, classes, vert_loc, lon_loc, lat_loc)


def join_kernel(*refs):
    *pieces, out_ref = refs
    for l in range(out_ref.shape[0]):
        total = pieces[0][l].astype(F32)
        for piece in pieces[1:]:
            total += piece[l].astype(F32)
        out_ref[l] = total.astype(BF16)


def join(pieces):
    vmem = pl.BlockSpec(memory_space=pltpu.VMEM)
    return pl.pallas_call(
        join_kernel,
        in_specs=[vmem] * len(pieces),
        out_specs=vmem,
        out_shape=jax.ShapeDtypeStruct(pieces[0].shape, BF16),
        compiler_params=pltpu.CompilerParams(vmem_limit_bytes=8 * 1024 * 1024),
        name="join",
    )(*pieces)


def weigh_kernel(precision_ref, *refs):
    *pieces, out_ref = refs
    for l in range(out_ref.shape[0]):
        total = pieces[0][l].astype(F32)
        for piece in pieces[1:]:
            total += piece[l].astype(F32)
        out_ref[l] = (total * precision_ref[l]).astype(BF16)


def weigh(precision, pieces):
    vmem = pl.BlockSpec(memory_space=pltpu.VMEM)
    return pl.pallas_call(
        weigh_kernel,
        in_specs=[vmem] * (1 + len(pieces)),
        out_specs=vmem,
        out_shape=jax.ShapeDtypeStruct(pieces[0].shape, BF16),
        compiler_params=pltpu.CompilerParams(vmem_limit_bytes=8 * 1024 * 1024),
        name="weigh",
    )(precision, *pieces)


def spread_out_kernel(first, *refs):
    pieces = CORE * Y
    weights, kept, refs = refs[:pieces], refs[pieces], refs[pieces + 1 :]
    big_ref, lon_ref, outs = refs[0], refs[1], refs[2 : 2 + LATS]
    adj, mixed = refs[2 + LATS :]
    levels, rows, cols = adj.shape
    step = levels // pieces
    share = cols // LATS

    def member(k):
        for low in range(0, rows, 16):
            for n, piece in enumerate(weights):
                for i in range(step):
                    own = kept[n // Y, -n % Y, first + k, i, low : low + 16, :]
                    weight = piece[i, low : low + 16, :]
                    adj[n * step + i, low : low + 16, :] = own.astype(F32) * weight.astype(F32)
            for at in range(low, low + 16, 8):
                x = adj[:, at : at + 8, :].reshape(levels * 8, cols).astype(BF16)
                y = jnp.dot(big_ref[...], x, preferred_element_type=F32)
                mixed[:, at : at + 8, :] = y.reshape(levels, 8, cols)
        block = 256 // rows
        for n in range(levels // block):
            x = mixed[block * n : block * n + block].reshape(256, cols).astype(BF16)
            y = nt_dot(lon_ref[...], x).astype(BF16)
            for d, out in enumerate(outs):
                out[k, :, 256 * n : 256 * n + 256] = y[share * d : share * d + share]

    count = outs[0].shape[0]
    if count == 1:
        member(0)
    else:
        pl.loop(0, count)(member)


def spread_out(weights, kept, big, lon, first, count):
    levels = len(weights) * weights[0].shape[0]
    _, rows, cols = weights[0].shape
    share = cols // LATS
    vmem = pl.BlockSpec(memory_space=pltpu.VMEM)
    args = (*weights, kept, big, lon)
    return pl.pallas_call(
        functools.partial(spread_out_kernel, first),
        in_specs=[vmem] * len(args),
        out_specs=[vmem] * LATS,
        out_shape=[jax.ShapeDtypeStruct((count, share, levels * rows), BF16)] * LATS,
        scratch_shapes=[pltpu.VMEM((levels, rows, cols), F32)] * 2,
        compiler_params=pltpu.CompilerParams(vmem_limit_bytes=24 * 1024 * 1024),
        cost_estimate=pl.CostEstimate(
            flops=count * 1_500_000_000, bytes_accessed=count * 2_500_000, transcendentals=0
        ),
        name="spread_out",
    )(*args)


def finish_kernel(here_ref, *refs):
    parts = refs[:LATS]
    turned_ref, out_ref = refs[LATS], refs[-1]
    share = parts[0].shape[1]
    groups = parts[0].shape[2] // 128
    lane = lax.broadcasted_iota(jnp.int32, (share, 128), 1) >> 5
    at = [lane == q for q in range(3)]
    for turn in range(EACH):
        lines = []
        for g in range(groups):
            sides = []
            for part in range(2):
                tiles = [
                    parts[EACH * part + (turn - q) % EACH][0, :, 128 * g : 128 * g + 128]
                    for q in range(EACH)
                ]
                side = tiles[3]
                for q in range(3):
                    side = jnp.where(at[q], tiles[q], side)
                sides.append(side)
            lines.append(jnp.concatenate(sides, axis=1))
        x = jnp.concatenate(lines, axis=0)
        y = nt_dot(x, turned_ref[turn]).astype(BF16)
        level = (turn + 8 - here_ref[2]) & 3
        for g in range(groups):
            out_ref[0, EACH * g + level] = y[share * g : share * g + share]


def finish(here, parts, turned, first, members, so_far=None):
    count, share, wide = parts[0].shape
    size = turned.shape[1]
    levels = wide // 32
    args = (*parts, turned) if so_far is None else (*parts, turned, so_far)
    extra = [] if so_far is None else [pl.BlockSpec(memory_space=pl.ANY)]
    return pl.pallas_call(
        finish_kernel,
        grid_spec=pltpu.PrefetchScalarGridSpec(
            num_scalar_prefetch=1,
            grid=(count,),
            in_specs=[pl.BlockSpec((1, share, wide), lambda k, s: (k, 0, 0))] * LATS
            + [pl.BlockSpec(turned.shape, lambda k, s: (0, 0, 0))]
            + extra,
            out_specs=pl.BlockSpec((1, levels, share, size), lambda k, s: (first + k, 0, 0, 0)),
        ),
        out_shape=jax.ShapeDtypeStruct((members, levels, share, size), BF16),
        input_output_aliases={} if so_far is None else {len(args): 0},
        compiler_params=pltpu.CompilerParams(
            dimension_semantics=("arbitrary",), vmem_limit_bytes=16 * 1024 * 1024
        ),
        cost_estimate=pl.CostEstimate(
            flops=count * 700_000_000, bytes_accessed=count * 2_500_000, transcendentals=0
        ),
        name="finish",
    )(here, *args)


def passed_on(axis, pieces, order):
    count = len(pieces)
    parts = [pieces[0]] + [None] * (count - 1)
    for d in order:
        parts[d] = lax.ppermute(pieces[d], axis, [(i, (i + d) % count) for i in range(count)])
    return parts


def local(controls, spread, classes, prec_table, vert_loc, lon_loc, lat_loc):
    controls = pltpu.with_memory_space_constraint(controls, pltpu.HBM)
    spread = pltpu.with_memory_space_constraint(spread, pltpu.HBM)
    members = spread.shape[0]
    here = jnp.stack([lax.axis_index(name) for name in ("core", "y", LAT)])
    swap = [(0, 1), (1, 0)]

    precision, big, lon, turned = tables(here, prec_table, classes, vert_loc, lon_loc, lat_loc)
    send, kept, own_controls = other_half(here, spread, controls)
    keep = own_half(kept, own_controls)
    arrived = lax.ppermute(send, "core", swap)
    pieces = chip_sum(keep, arrived)
    along_y = join(passed_on("y", pieces, range(1, Y)))
    along_z = passed_on("zh", [along_y] * ZH, Z_ORDER)
    weighted = weigh(precision, along_z)
    own = passed_on("y", [weighted] * Y, range(1, Y))
    weights = list(own)
    for x in own:
        weights.append(lax.ppermute(x, "core", swap))

    result = None
    for start, count in GROUPS:
        sending = spread_out(weights, kept, big, lon, start, count)
        parts = passed_on(LAT, sending, ORDER)
        result = finish(here, parts, turned, start, members, result)
    return result


def solution(mesh):
    finer = Mesh(
        mesh.devices.reshape(ZH, Y, CORE, mesh.shape["lat"]), ("zh", "y", "core", LAT)
    )
    members = P(("zh", "y", "core"), None, LAT, None)
    return jax.shard_map(
        local,
        mesh=finer,
        in_specs=(members, members, P(LAT, None), P(), P(), P(), P()),
        out_specs=members,
        check_vma=False,
    )
```
